768 devices in a mesh: blk: 192 (over x, y_lo, z), band: 4 (over y_hi, core).
Axes of the slice: x: 4, y: 8 (y_hi: 2, y_lo: 4; y = y_hi * 4 + y_lo), z: 12, core: 2. Of those that a mesh axis runs over, the one named last changes fastest.
Arguments:
- disp_fwd: float32 [192, 4, 25, 2048], P('blk', 'band'), may hold values from -6 to 6
- prev_fwd: float32 [192, 4, 25, 2048], P('blk', 'band'), may hold values from -6 to 6
- disp_adj: float32 [192, 4, 25, 2048], P('blk', 'band'), may hold values from -6 to 6
- prev_adj: float32 [192, 4, 25, 2048], P('blk', 'band'), may hold values from -6 to 6
- modulus: float32 [192, 4, 25, 2048], P('blk', 'band'), may hold values from 0.5 to 2
- radius: float32 [192, 4, 25], P('blk', 'band'), may hold values from 256 to 2048
- step_scale: float32 [192, 4, 25], P('blk', 'band'), may hold values from 0.01 to 0.04
- kernel_in: float32 [192, 4, 25, 2048], P('blk', 'band'), may hold values from -6 to 6
- buckets: int32 [192, 4], P('blk', 'band'), may hold values from 0 to 3
- halo_count: int32 [192, 4, 4], P('blk', 'band'), may hold values from 0 to 8, as said below
- blk_nodes: int32 [192, 4, 2, 8], P('blk', 'band'), may hold values from 0 to 24, as said below
- band_nodes: int32 [192, 4, 2, 4], P('blk', 'band'), may hold values from 0 to 24, as said below
Outputs:
- next_fwd: float32 [192, 4, 25, 2048], P('blk', 'band')
- next_adj: float32 [192, 4, 25, 2048], P('blk', 'band')
- kernel_out: float32 [192, 4, 25, 2048], P('blk', 'band')
The draws below stay inside these ranges and needn't reach their ends.
Inputs may be any that keep to these rules, and one draw needn't show every extreme that they name: `halo_count`: entries 0 and 1 count the nodes shared with the blk neighbour below and above, entries 2 and 3 with the band neighbour below and above. A device's count toward a neighbour equals the neighbour's count back; counts toward the outside of the grid are zero; some pair along blk shares 8 nodes and some pair along band 4. Slot k of a device's list toward a blk neighbour and slot k of that neighbour's list back hold copies of one node; slots at or past the count are unused. The 24 ids of one device over blk_nodes and band_nodes are all different. `band_nodes`: slot k of a device's list toward a band neighbour and slot k of that neighbour's list back hold copies of one node; slots at or past the count are unused; ids are different from those of blk_nodes on the same device.
All inputs are finite; a program needn't handle non-finite values.
Results may differ from the reference program's by a relative error of at most 0.0046.
Values sent between devices are 32-bit elements; how exact they have to be, the bound alone decides.
No kernel may reach another device: no remote copies, remote signals or barrier semaphores. Data moves between devices by JAX's collectives and lax.ppermute only.
A program may use at most 32 MiB of HBM per device.

```python
import math
import jax
import jax.numpy as jnp
import numpy as np
from jax import lax

MODES = 1024
COEFF = 2048
SAMPLES = 2048
NODES = 25
EL_DEV = 1
SHARED_Z = 4
SHARED_B = 8
GRID_B = 192
GRID_Z = 4
DEPTH = 4


def shuffle(single_key):
    return jax.random.permutation(single_key, EL_DEV * NODES).astype(jnp.int32)


def halo_plan(key):
    blk_key = jax.random.fold_in(key, 101)
    band_key = jax.random.fold_in(key, 202)
    counts_blk = jax.random.randint(jax.random.fold_in(blk_key, 1), (GRID_B - 1, GRID_Z), 1, SHARED_B + 1, dtype=jnp.int32)
    forced_blk = jax.random.randint(jax.random.fold_in(blk_key, 2), (), 0, (GRID_B - 1) * GRID_Z, dtype=jnp.int32)
    counts_blk = counts_blk.reshape(-1).at[forced_blk].set(SHARED_B).reshape(GRID_B - 1, GRID_Z)
    counts_band = jax.random.randint(jax.random.fold_in(band_key, 1), (GRID_B, GRID_Z - 1), 1, SHARED_Z + 1, dtype=jnp.int32)
    forced_band = jax.random.randint(jax.random.fold_in(band_key, 2), (), 0, GRID_B * (GRID_Z - 1), dtype=jnp.int32)
    counts_band = counts_band.reshape(-1).at[forced_band].set(SHARED_Z).reshape(GRID_B, GRID_Z - 1)
    zero_row = jnp.zeros((1, GRID_Z), jnp.int32)
    zero_col = jnp.zeros((GRID_B, 1), jnp.int32)
    lower_blk = jnp.concatenate([zero_row, counts_blk], axis=0)
    upper_blk = jnp.concatenate([counts_blk, zero_row], axis=0)
    lower_band = jnp.concatenate([zero_col, counts_band], axis=1)
    upper_band = jnp.concatenate([counts_band, zero_col], axis=1)
    counts = jnp.stack([lower_blk, upper_blk, lower_band, upper_band], axis=-1)
    perm_keys = jax.random.split(jax.random.fold_in(key, 303), GRID_B * GRID_Z)
    shuffled = jax.vmap(shuffle)(perm_keys)
    blk_lists = shuffled[:, :2 * SHARED_B].reshape(GRID_B, GRID_Z, 2, SHARED_B)
    band_lists = shuffled[:, 2 * SHARED_B:2 * SHARED_B + 2 * SHARED_Z].reshape(GRID_B, GRID_Z, 2, SHARED_Z)
    return (counts, blk_lists, band_lists)


def draw_halo_count(key, part):
    return halo_plan(key)[0]


def draw_blk_nodes(key, part):
    return halo_plan(key)[1]


def draw_band_nodes(key, part):
    return halo_plan(key)[2]


def with_ends(entries, stream_key, low, high):
    shape = entries.shape
    index_at = [jax.random.randint(jax.random.fold_in(stream_key, axis), (), 0, shape[axis]) for axis in range(len(shape))]
    entries = entries.at[tuple(index_at)].set(low)
    longest = shape.index(max(shape))
    index_at[longest] = (index_at[longest] + 1) % shape[longest]
    return entries.at[tuple(index_at)].set(high)


def shard_levels(key, shape, shards, low, top_value):
    def one(dim, blocks):
        heights = jax.random.uniform(jax.random.fold_in(jax.random.fold_in(key, 6), dim), (blocks,), jnp.float32, low / len(shards), top_value / len(shards))
        return jnp.repeat(jnp.exp(heights), shape[dim] // blocks).reshape((-1,) + (1,) * (len(shape) - dim - 1))

    gain = one(*shards[0])
    for cut in shards[1:]:
        gain = gain * one(*cut)
    return gain


def cumulative_ranks(amount, slope):
    loads = [(1 << 20) // math.isqrt(rank ** slope) + 1 for rank in range(1, amount + 1)]
    spread = 1 + sum(loads) // (1 << 30)
    return np.cumsum(np.array([max(1, weight // spread) for weight in loads]))


def ranked(rng, dims, count, slope):
    grid = cumulative_ranks(count, slope)
    lot = jax.random.randint(jax.random.fold_in(rng, 1), dims, 0, int(grid[count - 1]))
    rank = jnp.searchsorted(jnp.asarray(grid, jnp.int32), lot, side="right")
    return jax.random.permutation(jax.random.fold_in(rng, 2), count)[rank].astype(jnp.int32)


def scatter_about(own_key, extent, scale, limit, cuts=(), kind=jnp.bfloat16):
    entries = scale * jax.random.normal(own_key, extent, jnp.float32)
    if cuts:
        entries = entries * shard_levels(own_key, extent, cuts, -0.22, 0.18)
    return jnp.clip(entries, -limit, limit).astype(kind)


def setup_inputs(seed: int = 0) -> dict:
    splits = jax.random.split(jax.random.key(seed), 13)
    disp_fwd = scatter_about(splits[0], (GRID_B, DEPTH, NODES, COEFF), 1.0, 6.0, ((0, 192), (1, 4)), jnp.float32)
    prev_fwd = scatter_about(splits[1], (GRID_B, DEPTH, NODES, COEFF), 1.0, 6.0, ((0, 192), (1, 4)), jnp.float32)
    disp_adj = scatter_about(splits[2], (GRID_B, DEPTH, NODES, COEFF), 1.0, 6.0, ((0, 192), (1, 4)), jnp.float32)
    prev_adj = scatter_about(splits[3], (GRID_B, DEPTH, NODES, COEFF), 1.0, 6.0, ((0, 192), (1, 4)), jnp.float32)
    modulus = jnp.clip(jnp.exp(math.log(2.0) - 1.3862944 * jax.random.uniform(splits[4], (GRID_B, DEPTH, NODES, SAMPLES), jnp.float32) ** shard_levels(splits[4], (GRID_B, DEPTH, NODES, SAMPLES), ((0, 192), (1, 4)), -0.2, 0.2)), 0.5, 2.0)
    radius = jnp.clip(jnp.exp(math.log(2048.0) - 2.0794415 * jax.random.uniform(splits[5], (GRID_B, DEPTH, NODES), jnp.float32) ** shard_levels(splits[5], (GRID_B, DEPTH, NODES), ((0, 192), (1, 4)), -0.2, 0.2)), 256.0, 2048.0)
    step_scale = jnp.clip(jnp.exp(math.log(0.04) - 1.3862944 * jax.random.uniform(splits[6], (GRID_B, DEPTH, NODES), jnp.float32) ** shard_levels(splits[6], (GRID_B, DEPTH, NODES), ((0, 192), (1, 4)), -0.2, 0.2)), 0.01, 0.04)
    kernel_in = scatter_about(splits[7], (GRID_B, DEPTH, NODES, SAMPLES), 1.0, 6.0, ((0, 192), (1, 4)), jnp.float32)
    buckets = with_ends(ranked(splits[8], (GRID_B, DEPTH), 4, 2), jax.random.fold_in(splits[8], 3), 0, 3).astype(jnp.int32)
    halo_count = draw_halo_count(jax.random.fold_in(splits[12], 71), 0)
    blk_nodes = draw_blk_nodes(jax.random.fold_in(splits[12], 71), 0)
    band_nodes = draw_band_nodes(jax.random.fold_in(splits[12], 71), 0)
    return dict(disp_fwd=disp_fwd, prev_fwd=prev_fwd, disp_adj=disp_adj, prev_adj=prev_adj, modulus=modulus, radius=radius, step_scale=step_scale, kernel_in=kernel_in, buckets=buckets, halo_count=halo_count, blk_nodes=blk_nodes, band_nodes=band_nodes)


def gll_tables():
    inner_root = math.sqrt(3.0 / 7.0)
    points = np.array([-1.0, -inner_root, 0.0, inner_root, 1.0])
    weights = np.array([0.1, 49.0 / 90.0, 32.0 / 45.0, 49.0 / 90.0, 0.1])
    legendre = (35.0 * points ** 4 - 30.0 * points ** 2 + 3.0) / 8.0
    derivative = np.zeros((5, 5))
    for target in range(5):
        for source in range(5):
            if target != source:
                derivative[target, source] = legendre[target] / legendre[source] / (points[target] - points[source])
    derivative[0, 0] = -5.0
    derivative[4, 4] = 5.0
    return (jnp.asarray(derivative, jnp.float32), jnp.asarray(np.outer(weights, weights), jnp.float32))

def azimuth_table(mode_total):
    sample_len = 2 * mode_total
    table_shape = (2 * mode_total, sample_len)
    row_ids = lax.broadcasted_iota(jnp.int32, table_shape, 0)
    col_ids = lax.broadcasted_iota(jnp.int32, table_shape, 1)
    quarter = (row_ids >= mode_total).astype(jnp.int32) * (sample_len // 4)
    phase = (row_ids % mode_total * col_ids + quarter) % sample_len
    factor = math.sqrt(2.0 / sample_len)
    return (jnp.cos(phase.astype(jnp.float32) * (2.0 * math.pi / sample_len)) * factor).astype(jnp.bfloat16)

def mode_tops(mode_total):
    return [max(mode_total // 64, 1), max(mode_total // 16, 1), max(mode_total // 4, 1), mode_total]

def mode_mask(buckets, mode_total):
    order_tops = mode_tops(mode_total)
    order_limit = jnp.where(buckets == 0, order_tops[0], jnp.where(buckets == 1, order_tops[1], jnp.where(buckets == 2, order_tops[2], order_tops[3])))
    kept = (jnp.arange(mode_total, dtype=jnp.int32) < order_limit[..., None]).astype(jnp.float32)
    return jnp.concatenate([kept, kept], axis=-1)

def spin(coeffs, inv_radius, mode_orders):
    half_len = mode_orders.shape[0]
    return jnp.concatenate([-mode_orders * coeffs[..., half_len:], mode_orders * coeffs[..., :half_len]], axis=-1) * inv_radius

def unspin(coeffs, inv_radius, mode_orders):
    half_len = mode_orders.shape[0]
    return jnp.concatenate([mode_orders * coeffs[..., half_len:], -mode_orders * coeffs[..., :half_len]], axis=-1) * inv_radius

def field_terms(coeffs, inv_radius, weight, azim_table, derivative):
    element_total = coeffs.shape[0]
    coeff_len = coeffs.shape[-1]
    sample_len = azim_table.shape[1]
    mode_orders = jnp.arange(coeff_len // 2, dtype=jnp.float32)
    physical = jnp.dot(coeffs.astype(jnp.bfloat16).reshape(-1, coeff_len), azim_table, preferred_element_type=jnp.float32).reshape(element_total, 5, 5, sample_len)
    spun_low = spin(coeffs, inv_radius, mode_orders).astype(jnp.bfloat16).reshape(-1, coeff_len)
    azimuthal = jnp.dot(spun_low, azim_table, preferred_element_type=jnp.float32).reshape(element_total, 5, 5, sample_len)
    grad_s = jnp.einsum('ab,ebjk->eajk', derivative, physical, precision=lax.Precision.HIGHEST)
    grad_z = jnp.einsum('ab,eibk->eiak', derivative, physical, precision=lax.Precision.HIGHEST)
    diverge = jnp.einsum('ba,ebjk->eajk', derivative, weight * grad_s, precision=lax.Precision.HIGHEST) + jnp.einsum('ba,eibk->eiak', derivative, weight * grad_z, precision=lax.Precision.HIGHEST)
    contract_dims = (((1,), (1,)), ((), ()))
    back_div = lax.dot_general(diverge.astype(jnp.bfloat16).reshape(-1, sample_len), azim_table, contract_dims, preferred_element_type=jnp.float32).reshape(element_total, 25, coeff_len)
    back_phi = lax.dot_general((weight * azimuthal).astype(jnp.bfloat16).reshape(-1, sample_len), azim_table, contract_dims, preferred_element_type=jnp.float32).reshape(element_total, 25, coeff_len)
    stiff = back_div + unspin(back_phi, inv_radius, mode_orders)
    return (stiff, grad_s, grad_z, azimuthal)

def pick_rows(table, nodes):
    return table[nodes]

def add_rows(target, nodes, values):
    return target.at[nodes].add(values)

def reference(disp_fwd, prev_fwd, disp_adj, prev_adj, modulus, radius, step_scale, kernel_in, buckets, halo_count, blk_nodes, band_nodes):
    derivative, quadrature = gll_tables()
    azim_table = azimuth_table(MODES)

    def column(inputs):
        col_fwd, col_adj, col_mod, col_rad, col_bucket, col_kernel = inputs
        kept = mode_mask(col_bucket, MODES)[:, None, :]
        inv_radius = 1.0 / col_rad[..., None]
        weight = col_mod.reshape(-1, 5, 5, SAMPLES) * quadrature[None, :, :, None]
        stiff_fwd, fwd_s, fwd_z, fwd_p = field_terms(col_fwd * kept, inv_radius, weight, azim_table, derivative)
        stiff_adj, adj_s, adj_z, adj_p = field_terms(col_adj * kept, inv_radius, weight, azim_table, derivative)
        products = fwd_s * adj_s + fwd_z * adj_z + fwd_p * adj_p
        kernel = col_kernel - (quadrature[None, :, :, None] * products).reshape(-1, NODES, SAMPLES)
        return (stiff_fwd * kept, stiff_adj * kept, kernel)
    stiff_fwd, stiff_adj, kernel_out = lax.map(column, (disp_fwd, disp_adj, modulus, radius, buckets, kernel_in))

    def assemble(stiff):
        local = stiff.reshape(GRID_B, GRID_Z, EL_DEV * NODES, COEFF)
        picker = jax.vmap(jax.vmap(pick_rows))
        placer = jax.vmap(jax.vmap(add_rows))
        blk_slots = jnp.arange(SHARED_B, dtype=jnp.int32)
        band_slots = jnp.arange(SHARED_Z, dtype=jnp.int32)
        total = local
        sends = picker(local, blk_nodes[:, :, 1])
        arrived = jnp.concatenate([jnp.zeros_like(sends[:1]), sends[:-1]], axis=0)
        valid = (blk_slots[None, None, :] < halo_count[:, :, 0:1]).astype(jnp.float32)[..., None]
        total = placer(total, blk_nodes[:, :, 0], arrived * valid)
        sends = picker(local, blk_nodes[:, :, 0])
        arrived = jnp.concatenate([sends[1:], jnp.zeros_like(sends[:1])], axis=0)
        valid = (blk_slots[None, None, :] < halo_count[:, :, 1:2]).astype(jnp.float32)[..., None]
        total = placer(total, blk_nodes[:, :, 1], arrived * valid)
        sends = picker(local, band_nodes[:, :, 1])
        arrived = jnp.concatenate([jnp.zeros_like(sends[:, :1]), sends[:, :-1]], axis=1)
        valid = (band_slots[None, None, :] < halo_count[:, :, 2:3]).astype(jnp.float32)[..., None]
        total = placer(total, band_nodes[:, :, 0], arrived * valid)
        sends = picker(local, band_nodes[:, :, 0])
        arrived = jnp.concatenate([sends[:, 1:], jnp.zeros_like(sends[:, :1])], axis=1)
        valid = (band_slots[None, None, :] < halo_count[:, :, 3:4]).astype(jnp.float32)[..., None]
        total = placer(total, band_nodes[:, :, 1], arrived * valid)
        return total.reshape(GRID_B, DEPTH, NODES, COEFF)
    kept_all = mode_mask(buckets, MODES)[:, :, None, :]
    growth = step_scale[..., None]
    next_fwd = kept_all * (2.0 * (disp_fwd * kept_all) - prev_fwd - growth * assemble(stiff_fwd))
    next_adj = kept_all * (2.0 * (disp_adj * kept_all) - prev_adj - growth * assemble(stiff_adj))
    return (next_fwd, next_adj, kernel_out)
```

```python
import math

import jax
import jax.numpy as jnp
import numpy as np
from jax import lax
from jax.experimental import pallas as pl
from jax.experimental.pallas import tpu as pltpu
from jax.sharding import PartitionSpec as P

NODES = 25
ROWS = 56
PITCH = 40
LANES = 128


def shifted(value, axis, steps):
    count = lax.axis_size(axis)
    initial, last = (max(0, -steps), min(count, count - steps))
    return lax.ppermute(value, axis, [(source, source + steps) for source in range(initial, last)])


def gll_tables():
    inner_root = math.sqrt(3.0 / 7.0)
    points = np.array([-1.0, -inner_root, 0.0, inner_root, 1.0])
    weights = np.array([0.1, 49.0 / 90.0, 32.0 / 45.0, 49.0 / 90.0, 0.1])
    legendre = (35.0 * points**4 - 30.0 * points**2 + 3.0) / 8.0
    derivative = np.zeros((5, 5))
    for target in range(5):
        for source in range(5):
            if target != source:
                derivative[target, source] = (
                    legendre[target] / legendre[source] / (points[target] - points[source])
                )
    derivative[0, 0] = -5.0
    derivative[4, 4] = 5.0
    return derivative, np.outer(weights, weights)


DERIV, QUAD = gll_tables()


def transform_tables():
    lane = np.arange(LANES)
    sample = 8 * (lane % 16) + lane // 16
    angle = 2.0 * np.pi * ((np.arange(LANES)[:, None] * sample[None, :]) % LANES) / LANES
    table = np.concatenate([np.cos(angle), -np.sin(angle)], axis=0) / 32.0
    turn = 2.0 * np.pi * np.arange(16)[:, None] * lane[None, :] / 2048.0
    twiddle = np.concatenate([np.cos(turn), np.sin(turn)], axis=0)
    return table, twiddle


def times_root(z, eighth, sign):
    re, im = z
    root = math.sqrt(0.5)
    if eighth == 0:
        return z
    if eighth == 1:
        return ((re - im) * root, (re + im) * root) if sign > 0 else ((re + im) * root, (im - re) * root)
    if eighth == 2:
        return (-im, re) if sign > 0 else (im, -re)
    return ((-re - im) * root, (re - im) * root) if sign > 0 else ((im - re) * root, (-re - im) * root)


def plus(x, y):
    return (x[0] + y[0], x[1] + y[1])


def minus(x, y):
    return (x[0] - y[0], x[1] - y[1])


def plus_turned(x, y, sign):
    return (x[0] - y[1], x[1] + y[0]) if sign > 0 else (x[0] + y[1], x[1] - y[0])


def dft4(a, b, c, d, sign):
    s, t, u, v = plus(a, c), minus(a, c), plus(b, d), minus(b, d)
    return [plus(s, u), plus_turned(t, v, sign), minus(s, u), plus_turned(t, v, -sign)]


def dft8(z, sign):
    even = dft4(z[0], z[2], z[4], z[6], sign)
    odd = dft4(z[1], z[3], z[5], z[7], sign)
    low, high = [], []
    for k in range(4):
        if k == 2:
            low.append(plus_turned(even[k], odd[k], sign))
            high.append(plus_turned(even[k], odd[k], -sign))
        else:
            turned = times_root(odd[k], k, sign)
            low.append(plus(even[k], turned))
            high.append(minus(even[k], turned))
    return low + high


def times_const(z, angle):
    c, s = math.cos(angle), math.sin(angle)
    return (z[0] * c - z[1] * s, z[0] * s + z[1] * c)


def spread(z):
    even = dft8(z, 1)
    odd = dft8([z[0]] + [times_const(z[m], math.pi * m / 8.0) for m in range(1, 8)], 1)
    return [(even, odd)[k % 2][k // 2] for k in range(16)]


def gathered(v):
    even = dft8(v[0::2], -1)
    odd = dft8(v[1::2], -1)
    return [plus(even[m], times_const(odd[m], -math.pi * m / 8.0) if m else odd[m]) for m in range(8)]


def centred(table, p):
    e0, o0, e1, o1, c = p[0] + p[4], p[0] - p[4], p[1] + p[3], p[1] - p[3], p[2]
    out = [None] * 5
    for i in range(2):
        t = table[i]
        odd = o0 * float(0.5 * (t[0] - t[4])) + o1 * float(0.5 * (t[1] - t[3]))
        even = e0 * float(0.5 * (t[0] + t[4])) + e1 * float(0.5 * (t[1] + t[3])) + c * float(t[2])
        out[i], out[4 - i] = odd + even, odd - even
    out[2] = o0 * float(table[2, 0]) + o1 * float(table[2, 1])
    return out


def swap_blocks(x):
    lane = lax.broadcasted_iota(jnp.int32, x[0].shape, 1)
    for bit in (8, 4, 2, 1):
        clear = (lane & bit) == 0
        for s in range(16):
            if s & bit:
                continue
            a, b = x[s], x[s | bit]
            x[s] = jnp.where(clear, a, pltpu.roll(b, bit, 1))
            x[s | bit] = jnp.where(clear, pltpu.roll(a, LANES - bit, 1), b)
    return x


def order_limit(bucket):
    return jnp.where(bucket == 0, 16, jnp.where(bucket == 1, 64, jnp.where(bucket == 2, 256, 1024)))


def stiffness_kernel(
    bucket_ref, blk_ref, band_ref, radius_ref, twiddle_ref, table_ref, back_ref, fwd_hbm, adj_hbm, mod_hbm,
    stiff_ref, waves_ref, blk_low_ref, blk_high_ref, band_low_ref, band_high_ref,
    field, mod, weight, stress, inv, sems,
):
    loads = [
        pltpu.make_async_copy(fwd_hbm, field.at[pl.ds(0, 400)], sems.at[0]),
        pltpu.make_async_copy(adj_hbm, field.at[pl.ds(400, 400)], sems.at[1]),
        pltpu.make_async_copy(mod_hbm, mod.at[pl.ds(0, 400)], sems.at[2]),
    ]
    for load in loads:
        load.start()
    limit = order_limit(bucket_ref[0, 0])
    lane8 = lax.broadcasted_iota(jnp.int32, (8, LANES), 1)
    orders = [(lane8 + 128 * a).astype(jnp.float32) for a in range(8)]

    row = lax.broadcasted_iota(jnp.int32, (ROWS, LANES), 0)
    node = jnp.where(row >= NODES, row - NODES, row)
    lane = lax.broadcasted_iota(jnp.int32, (ROWS, LANES), 1)
    radius = jnp.broadcast_to(radius_ref[0:1, :], (ROWS, LANES))
    radius = jnp.sum(jnp.where(lane == node, radius, 0.0), axis=1, keepdims=True)
    inv[...] = jnp.broadcast_to(1.0 / jnp.where(radius > 0.0, radius, 1.0), (ROWS, LANES))
    loads[0].wait()
    loads[1].wait()

    def forward(g, carry):
        inv_r = inv[pl.ds(pl.multiple_of(8 * g, 8), 8), :]
        base = 128 * g
        u, w = [], []
        for a in range(8):
            kept = (lane8 + 128 * a) < limit
            re = jnp.where(kept, field[pl.ds(base + a, 8, stride=16), :], 0.0)
            im = jnp.where(kept, field[pl.ds(base + 8 + a, 8, stride=16), :], 0.0)
            scale = orders[a]
            w.append((-(scale * im) * inv_r, (scale * re) * inv_r))
            u.append((re, im))
        res, ims = [], []
        for z in (u, w):
            z = [tuple(part.astype(jnp.bfloat16).astype(jnp.float32) for part in term) for term in z]
            for c, (re, im) in enumerate(spread(z)):
                if c:
                    cos, sin = twiddle_ref[c : c + 1, :], twiddle_ref[16 + c : 17 + c, :]
                    re, im = re * cos - im * sin, re * sin + im * cos
                res.append(re)
                ims.append(im)
        lhs = jnp.concatenate([jnp.concatenate(res, axis=0), jnp.concatenate(ims, axis=0)], axis=1)
        out = jnp.dot(lhs.astype(jnp.bfloat16), table_ref[...], preferred_element_type=jnp.float32)
        for t in range(2):
            for c in range(16):
                at = pl.multiple_of(ROWS * c + 8 * g, 8)
                waves_ref[t, pl.ds(at, 8), :] = out[128 * t + 8 * c : 128 * t + 8 * c + 8]
        return carry

    lax.fori_loop(0, ROWS // 8, forward, 0)
    loads[2].wait()

    def reorder(g, carry):
        x = swap_blocks([mod[pl.ds(128 * g + s, 8, stride=16), :] for s in range(16)])
        for c in range(16):
            weight[pl.ds(pl.multiple_of(PITCH * c + 8 * g, 8), 8), :] = x[c]
        return carry

    lax.fori_loop(0, 4, reorder, 0)

    def stencil(step, carry):
        half, f = step // 2, step % 2
        top = ROWS * 8 * half + NODES * f
        w = [
            [weight[pl.ds(PITCH * 8 * half + 5 * i + j, 8, stride=PITCH), :] * float(QUAD[i, j]) for j in range(5)]
            for i in range(5)
        ]
        p = [[waves_ref[0, pl.ds(top + 5 * i + j, 8, stride=ROWS), :] for j in range(5)] for i in range(5)]
        total = []
        for i in range(5):
            grad = centred(DERIV, p[i])
            total.append(centred(DERIV.T, [w[i][j] * grad[j] for j in range(5)]))
        for j in range(5):
            grad = centred(DERIV, [p[i][j] for i in range(5)])
            part = centred(DERIV.T, [w[i][j] * grad[i] for i in range(5)])
            for i in range(5):
                stress[0, pl.ds(top + 5 * i + j, 8, stride=ROWS), :] = total[i][j] + part[i]
        for i in range(5):
            for j in range(5):
                at = pl.ds(top + 5 * i + j, 8, stride=ROWS)
                stress[1, at, :] = w[i][j] * waves_ref[1, at, :]
        return carry

    lax.fori_loop(0, 4, stencil, 0)

    def backward(g, carry):
        inv_r = inv[pl.ds(pl.multiple_of(8 * g, 8), 8), :]
        rows = [
            stress[t, pl.ds(pl.multiple_of(ROWS * c + 8 * g, 8), 8), :] for t in range(2) for c in range(16)
        ]
        lhs = jnp.concatenate(rows, axis=0).astype(jnp.bfloat16)
        out = jnp.dot(lhs, back_ref[...], preferred_element_type=jnp.float32)
        terms = []
        for t in range(2):
            v = []
            for c in range(16):
                at = 128 * t + 8 * c
                re, im = out[at : at + 8, :LANES], out[at : at + 8, LANES:]
                if c:
                    cos, sin = twiddle_ref[c : c + 1, :], twiddle_ref[16 + c : 17 + c, :]
                    re, im = re * cos + im * sin, im * cos - re * sin
                v.append((re, im))
            terms.append(gathered(v))
        for a in range(8):
            kept = (lane8 + 128 * a) < limit
            scale = orders[a]
            re = terms[0][a][0] + (scale * terms[1][a][1]) * inv_r
            im = terms[0][a][1] - (scale * terms[1][a][0]) * inv_r
            stiff_ref[pl.ds(128 * g + a, 8, stride=16), :] = jnp.where(kept, re, 0.0)
            stiff_ref[pl.ds(128 * g + 8 + a, 8, stride=16), :] = jnp.where(kept, im, 0.0)
        return carry

    lax.fori_loop(0, ROWS // 8, backward, 0)

    for ids, side, slots, out_ref in (
        (blk_ref, 0, 8, blk_low_ref), (blk_ref, 1, 8, blk_high_ref),
        (band_ref, 0, 4, band_low_ref), (band_ref, 1, 4, band_high_ref),
    ):
        for k in range(slots):
            at = ids[side, k] * 16
            for f in range(2):
                out_ref[pl.ds((f * slots + k) * 16, 16), :] = stiff_ref[pl.ds(pl.multiple_of(at + 400 * f, 16), 16), :]


def local_kernel(
    bucket_ref, scale_ref, waves_ref, stiff_ref, fwd_ref, adj_ref, prev_fwd_ref, prev_adj_ref, kernel_ref,
    base_ref, out_ref, slab,
):
    limit = order_limit(bucket_ref[0, 0])
    slot = lax.broadcasted_iota(jnp.int32, (16, LANES), 0)
    order = lax.broadcasted_iota(jnp.int32, (16, LANES), 1) + 128 * (slot % 8)
    kept = order < limit

    def update(n, carry):
        growth = scale_ref[0, n]
        at = pl.multiple_of(16 * n, 16)
        for f, (disp, prev) in enumerate(((fwd_ref, prev_fwd_ref), (adj_ref, prev_adj_ref))):
            rows = pl.ds(at, 16)
            both = pl.ds(pl.multiple_of(at + 400 * f, 16), 16)
            value = 2.0 * disp[rows, :] - prev[rows, :] - growth * stiff_ref[both, :]
            base_ref[both, :] = jnp.where(kept, value, 0.0)
        return carry

    lax.fori_loop(0, NODES, update, 0, unroll=5)

    for half in range(2):
        top = ROWS * 8 * half
        p = [
            [[waves_ref[0, pl.ds(top + NODES * f + 5 * i + j, 8, stride=ROWS), :] for j in range(5)] for i in range(5)]
            for f in range(2)
        ]
        total = [
            [
                waves_ref[1, pl.ds(top + 5 * i + j, 8, stride=ROWS), :]
                * waves_ref[1, pl.ds(top + NODES + 5 * i + j, 8, stride=ROWS), :]
                for j in range(5)
            ]
            for i in range(5)
        ]
        for i in range(5):
            fwd, adj = centred(DERIV, p[0][i]), centred(DERIV, p[1][i])
            for j in range(5):
                total[i][j] = total[i][j] + fwd[j] * adj[j]
        for j in range(5):
            fwd, adj = (centred(DERIV, [p[f][i][j] for i in range(5)]) for f in range(2))
            for i in range(5):
                slab[pl.ds(PITCH * 8 * half + 5 * i + j, 8, stride=PITCH), :] = (
                    total[i][j] + fwd[i] * adj[i]
                ) * float(QUAD[i, j])

    def finish(g, carry):
        x = swap_blocks([slab[pl.ds(pl.multiple_of(PITCH * c + 8 * g, 8), 8), :] for c in range(16)])
        for s in range(16):
            at = pl.ds(128 * g + s, 8, stride=16)
            out_ref[at, :] = kernel_ref[at, :] - x[s]
        return carry

    lax.fori_loop(0, 3, finish, 0)
    x = swap_blocks([slab[pl.ds(PITCH * c + 24, 1), :] for c in range(16)])
    for s in range(16):
        out_ref[pl.ds(384 + s, 1), :] = kernel_ref[pl.ds(384 + s, 1), :] - x[s]


def join_kernel(
    bucket_ref, count_ref, blk_ref, band_ref, scale_ref, base_ref, below_ref, above_ref, band_below_ref, band_above_ref,
    fwd_ref, adj_ref,
):
    limit = order_limit(bucket_ref[0, 0])
    slot = lax.broadcasted_iota(jnp.int32, (16, LANES), 0)
    order = lax.broadcasted_iota(jnp.int32, (16, LANES), 1) + 128 * (slot % 8)
    kept = order < limit
    outs = (fwd_ref, adj_ref)
    for f in range(2):
        outs[f][...] = base_ref[pl.ds(400 * f, 400), :]
    for side, ids, lane_side, slots, got in (
        (0, blk_ref, 0, 8, below_ref), (1, blk_ref, 1, 8, above_ref),
        (2, band_ref, 0, 4, band_below_ref), (3, band_ref, 1, 4, band_above_ref),
    ):
        for k in range(slots):
            node = ids[lane_side, k]
            take = jnp.logical_and(kept, k < count_ref[0, side])
            growth = scale_ref[0, node]
            at = pl.ds(pl.multiple_of(16 * node, 16), 16)
            for f in range(2):
                step = growth * got[pl.ds((f * slots + k) * 16, 16), :]
                outs[f][at, :] = outs[f][at, :] - jnp.where(take, step, 0.0)


def smem():
    return pl.BlockSpec(memory_space=pltpu.SMEM)


def vmem():
    return pl.BlockSpec(memory_space=pltpu.VMEM)


def anywhere():
    return pl.BlockSpec(memory_space=pl.ANY)


def shape(*dims):
    return jax.ShapeDtypeStruct(dims, jnp.float32)


def per_device(
    disp_fwd, prev_fwd, disp_adj, prev_adj, modulus, radius, step_scale, kernel_in, buckets, halo_count,
    blk_nodes, band_nodes,
):
    flat = lambda value: value.reshape(16 * NODES, LANES)
    table, twiddle = transform_tables()
    fwd, adj = flat(disp_fwd), flat(disp_adj)
    bucket, blk, band = buckets.reshape(1, 1), blk_nodes.reshape(2, 8), band_nodes.reshape(2, 4)
    scale = step_scale.reshape(1, NODES)
    line = jnp.pad(radius.reshape(1, NODES), ((0, 0), (0, LANES - NODES)))
    stiff, waves, blk_low, blk_high, band_low, band_high = pl.pallas_call(
        stiffness_kernel,
        out_shape=(
            shape(16 * ROWS, LANES), shape(2, 16 * ROWS, LANES), shape(256, LANES), shape(256, LANES),
            shape(128, LANES), shape(128, LANES),
        ),
        in_specs=[smem(), smem(), smem(), vmem(), vmem(), vmem(), vmem(), anywhere(), anywhere(), anywhere()],
        out_specs=(vmem(),) * 6,
        scratch_shapes=[
            pltpu.VMEM((16 * ROWS, LANES), jnp.float32),
            pltpu.VMEM((512, LANES), jnp.float32),
            pltpu.VMEM((16 * PITCH, LANES), jnp.float32),
            pltpu.VMEM((2, 16 * ROWS, LANES), jnp.float32),
            pltpu.VMEM((ROWS, LANES), jnp.float32),
            pltpu.SemaphoreType.DMA((3,)),
        ],
        cost_estimate=pl.CostEstimate(flops=500_000_000, bytes_accessed=3_000_000, transcendentals=0),
        name="stiffness",
    )(
        bucket, blk, band, line, jnp.asarray(twiddle, jnp.float32), jnp.asarray(table, jnp.bfloat16),
        jnp.asarray(table.T, jnp.bfloat16), fwd, adj, flat(modulus),
    )
    from_below = shifted(blk_high, "blk", 1)
    from_above = shifted(blk_low, "blk", -1)
    band_below = shifted(band_high, "band", 1)
    band_above = shifted(band_low, "band", -1)
    base, kernel_out = pl.pallas_call(
        local_kernel,
        out_shape=(shape(800, LANES), shape(400, LANES)),
        in_specs=[smem(), smem()] + [vmem()] * 7,
        out_specs=(vmem(), vmem()),
        scratch_shapes=[pltpu.VMEM((16 * PITCH, LANES), jnp.float32)],
        cost_estimate=pl.CostEstimate(flops=100_000_000, bytes_accessed=3_000_000, transcendentals=0),
        name="local",
    )(bucket, scale, waves, stiff, fwd, adj, flat(prev_fwd), flat(prev_adj), flat(kernel_in))
    next_fwd, next_adj = pl.pallas_call(
        join_kernel,
        out_shape=(shape(400, LANES), shape(400, LANES)),
        in_specs=[smem()] * 5 + [vmem()] * 5,
        out_specs=(vmem(), vmem()),
        cost_estimate=pl.CostEstimate(flops=1_000_000, bytes_accessed=1_500_000, transcendentals=0),
        name="join",
    )(
        bucket, halo_count.reshape(1, 4), blk, band, scale, base, from_below, from_above, band_below, band_above
    )
    return tuple(value.reshape(disp_fwd.shape) for value in (next_fwd, next_adj, kernel_out))


def solution(mesh):
    wide = P("blk", "band", None, None)
    line = P("blk", "band", None)
    in_specs = (wide,) * 5 + (line, line, wide, P("blk", "band"), line, wide, wide)
    return jax.shard_map(
        per_device, mesh=mesh, in_specs=in_specs, out_specs=(wide, wide, wide), check_vma=False
    )
```

```python
import math

import jax
import jax.numpy as jnp
import numpy as np
from jax import lax
from jax.experimental import pallas as pl
from jax.experimental.pallas import tpu as pltpu
from jax.sharding import PartitionSpec as P


NODES = 25
ROWS = 56
PITCH = 40
RUN = 12
LANES = 128


def gll_tables():
    inner_root = math.sqrt(3.0 / 7.0)
    points = np.array([-1.0, -inner_root, 0.0, inner_root, 1.0])
    weights = np.array([0.1, 49.0 / 90.0, 32.0 / 45.0, 49.0 / 90.0, 0.1])
    legendre = (35.0 * points**4 - 30.0 * points**2 + 3.0) / 8.0
    derivative = np.zeros((5, 5))
    for target in range(5):
        for source in range(5):
            if target != source:
                derivative[target, source] = (
                    legendre[target] / legendre[source] / (points[target] - points[source])
                )
    derivative[0, 0] = -5.0
    derivative[4, 4] = 5.0
    return derivative, np.outer(weights, weights)


DERIV, QUAD = gll_tables()


def transform_tables():
    lane = np.arange(LANES)
    sample = 8 * (lane % 16) + lane // 16
    angle = 2.0 * np.pi * ((np.arange(LANES)[:, None] * sample[None, :]) % LANES) / LANES
    table = np.concatenate([np.cos(angle), -np.sin(angle)], axis=0) / 32.0
    turn = 2.0 * np.pi * np.arange(16)[:, None] * lane[None, :] / 2048.0
    twiddle = np.concatenate([np.cos(turn), np.sin(turn)], axis=0)
    return table, twiddle


def times_root(z, eighth, sign):
    re, im = z
    root = math.sqrt(0.5)
    if eighth == 0:
        return z
    if eighth == 1:
        return ((re - im) * root, (re + im) * root) if sign > 0 else ((re + im) * root, (im - re) * root)
    if eighth == 2:
        return (-im, re) if sign > 0 else (im, -re)
    return ((-re - im) * root, (re - im) * root) if sign > 0 else ((im - re) * root, (-re - im) * root)


def plus(x, y):
    return (x[0] + y[0], x[1] + y[1])


def minus(x, y):
    return (x[0] - y[0], x[1] - y[1])


def plus_turned(x, y, sign):
    return (x[0] - y[1], x[1] + y[0]) if sign > 0 else (x[0] + y[1], x[1] - y[0])


def dft4(a, b, c, d, sign):
    s, t, u, v = plus(a, c), minus(a, c), plus(b, d), minus(b, d)
    return [plus(s, u), plus_turned(t, v, sign), minus(s, u), plus_turned(t, v, -sign)]


def dft8(z, sign):
    even = dft4(z[0], z[2], z[4], z[6], sign)
    odd = dft4(z[1], z[3], z[5], z[7], sign)
    low, high = [], []
    for k in range(4):
        if k == 2:
            low.append(plus_turned(even[k], odd[k], sign))
            high.append(plus_turned(even[k], odd[k], -sign))
        else:
            turned = times_root(odd[k], k, sign)
            low.append(plus(even[k], turned))
            high.append(minus(even[k], turned))
    return low + high


def times_const(z, angle):
    c, s = math.cos(angle), math.sin(angle)
    return (z[0] * c - z[1] * s, z[0] * s + z[1] * c)


def spread(z):
    even = dft8(z, 1)
    odd = dft8([z[0]] + [times_const(z[m], math.pi * m / 8.0) for m in range(1, 8)], 1)
    return [(even, odd)[k % 2][k // 2] for k in range(16)]


def gathered(v):
    even = dft8(v[0::2], -1)
    odd = dft8(v[1::2], -1)
    return [plus(even[m], times_const(odd[m], -math.pi * m / 8.0) if m else odd[m]) for m in range(8)]


def centred(table, p):
    e0, o0, e1, o1, c = p[0] + p[4], p[0] - p[4], p[1] + p[3], p[1] - p[3], p[2]
    out = [None] * 5
    for i in range(2):
        t = table[i]
        odd = o0 * float(0.5 * (t[0] - t[4])) + o1 * float(0.5 * (t[1] - t[3]))
        even = e0 * float(0.5 * (t[0] + t[4])) + e1 * float(0.5 * (t[1] + t[3])) + c * float(t[2])
        out[i], out[4 - i] = odd + even, odd - even
    out[2] = o0 * float(table[2, 0]) + o1 * float(table[2, 1])
    return out


def swap_blocks(x):
    lane = lax.broadcasted_iota(jnp.int32, x[0].shape, 1)
    for bit in (8, 4, 2, 1):
        clear = (lane & bit) == 0
        for s in range(16):
            if s & bit:
                continue
            a, b = x[s], x[s | bit]
            x[s] = jnp.where(clear, a, pltpu.roll(b, bit, 1))
            x[s | bit] = jnp.where(clear, pltpu.roll(a, LANES - bit, 1), b)
    return x


def order_limit(bucket):
    return jnp.where(bucket == 0, 16, jnp.where(bucket == 1, 64, jnp.where(bucket == 2, 256, 1024)))


def device_role():
    blk, band = lax.axis_index("blk"), lax.axis_index("band")
    return lax.rem(blk, RUN) == 0, lax.rem(blk, 2), lax.rem(band, 2)


def finish_locally(limit, scale_ref, waves_ref, stiff_ref, field_ref, late_ref, base_ref, slab, kout):
    slot = lax.broadcasted_iota(jnp.int32, (16, LANES), 0)
    order = lax.broadcasted_iota(jnp.int32, (16, LANES), 1) + 128 * (slot % 8)
    kept = order < limit

    def update(n, carry):
        growth = scale_ref[0, n]
        for f in range(2):
            rows = pl.ds(pl.multiple_of(16 * n + 400 * f, 16), 16)
            value = 2.0 * field_ref[rows, :] - late_ref[rows, :] - growth * stiff_ref[rows, :]
            base_ref[rows, :] = jnp.where(kept, value, 0.0)
        return carry

    lax.fori_loop(0, NODES, update, 0, unroll=5)

    def products(half, carry):
        top = ROWS * 8 * half
        p = [
            [[waves_ref[0, pl.ds(top + NODES * f + 5 * i + j, 8, stride=ROWS), :] for j in range(5)] for i in range(5)]
            for f in range(2)
        ]
        total = [
            [
                waves_ref[1, pl.ds(top + 5 * i + j, 8, stride=ROWS), :]
                * waves_ref[1, pl.ds(top + NODES + 5 * i + j, 8, stride=ROWS), :]
                for j in range(5)
            ]
            for i in range(5)
        ]
        for i in range(5):
            fwd, adj = centred(DERIV, p[0][i]), centred(DERIV, p[1][i])
            for j in range(5):
                total[i][j] = total[i][j] + fwd[j] * adj[j]
        for j in range(5):
            fwd, adj = (centred(DERIV, [p[f][i][j] for i in range(5)]) for f in range(2))
            for i in range(5):
                slab[pl.ds(PITCH * 8 * half + 5 * i + j, 8, stride=PITCH), :] = (
                    total[i][j] + fwd[i] * adj[i]
                ) * float(QUAD[i, j])
        return carry

    lax.fori_loop(0, 2, products, 0, unroll=True)

    def finish(g, carry):
        x = swap_blocks([slab[pl.ds(pl.multiple_of(PITCH * c + 8 * g, 8), 8), :] for c in range(16)])
        for s in range(16):
            at = 128 * g + s
            kout[pl.ds(at, 8, stride=16), :] = late_ref[pl.ds(800 + at, 8, stride=16), :] - x[s]
        return carry

    lax.fori_loop(0, 4, finish, 0, unroll=True)


def stiffness_kernel(
    bucket_ref, radius_ref, scale_ref, blk_ref, band_ref, twiddle_hbm, table_hbm, back_hbm, fwd_hbm, adj_hbm, mod_hbm,
    prev_fwd_hbm, prev_adj_hbm, kernel_hbm,
    stiff_ref, waves_ref, field, late, base_ref, odd_hbm, even_hbm, chip_hbm, far_hbm, out_hbm,
    mod, weight, stress, inv, twiddle_ref, table_ref, back_ref, slab, kout, odd_ref, even_ref, chip_ref, far_ref, sems,
):
    loads = [
        pltpu.make_async_copy(source, target, sems.at[i])
        for i, (source, target) in enumerate((
            (fwd_hbm, field.at[pl.ds(0, 400)]), (adj_hbm, field.at[pl.ds(400, 400)]), (twiddle_hbm, twiddle_ref),
            (table_hbm, table_ref), (mod_hbm, mod.at[pl.ds(0, 400)]), (back_hbm, back_ref),
            (prev_fwd_hbm, late.at[pl.ds(0, 400)]), (prev_adj_hbm, late.at[pl.ds(400, 400)]),
            (kernel_hbm, late.at[pl.ds(800, 400)]),
        ))
    ]
    for load in loads[:6]:
        load.start()
    limit = order_limit(bucket_ref[0, 0])
    first, odd, upper = device_role()
    lane8 = lax.broadcasted_iota(jnp.int32, (8, LANES), 1)
    orders = [(lane8 + 128 * a).astype(jnp.float32) for a in range(8)]

    inv[pl.ds(ROWS - 8, 8), :] = jnp.ones((8, LANES), jnp.float32)
    for n in range(NODES):
        line = jnp.full((1, LANES), radius_ref[0, n], jnp.float32)
        inv[pl.ds(n, 1), :] = line
        inv[pl.ds(NODES + n, 1), :] = line
    inv[...] = 1.0 / inv[...]
    for load in loads[:4]:
        load.wait()
    for load in loads[6:]:
        load.start()

    def forward(g, carry):
        inv_r = inv[pl.ds(pl.multiple_of(8 * g, 8), 8), :]
        base = 128 * g
        u, w = [], []
        for a in range(8):
            kept = (lane8 + 128 * a) < limit
            re = jnp.where(kept, field[pl.ds(base + a, 8, stride=16), :], 0.0)
            im = jnp.where(kept, field[pl.ds(base + 8 + a, 8, stride=16), :], 0.0)
            scale = orders[a]
            w.append((-(scale * im) * inv_r, (scale * re) * inv_r))
            u.append((re, im))
        res, ims = [], []
        for z in (u, w):
            z = [tuple(part.astype(jnp.bfloat16).astype(jnp.float32) for part in term) for term in z]
            for c, (re, im) in enumerate(spread(z)):
                if c:
                    cos, sin = twiddle_ref[c : c + 1, :], twiddle_ref[16 + c : 17 + c, :]
                    re, im = re * cos - im * sin, re * sin + im * cos
                res.append(re)
                ims.append(im)
        lhs = jnp.concatenate([jnp.concatenate(res, axis=0), jnp.concatenate(ims, axis=0)], axis=1)
        out = jnp.dot(lhs.astype(jnp.bfloat16), table_ref[...], preferred_element_type=jnp.float32)
        for t in range(2):
            for c in range(16):
                at = pl.multiple_of(ROWS * c + 8 * g, 8)
                waves_ref[t, pl.ds(at, 8), :] = out[128 * t + 8 * c : 128 * t + 8 * c + 8]
        return carry

    loads[4].wait()

    def reorder(g, carry):
        x = swap_blocks([mod[pl.ds(128 * g + s, 8, stride=16), :] for s in range(16)])
        for c in range(16):
            weight[pl.ds(pl.multiple_of(PITCH * c + 8 * g, 8), 8), :] = x[c]
        return carry

    lax.fori_loop(0, 4, lambda g, carry: reorder(g, forward(g, carry)), 0, unroll=True)
    lax.fori_loop(4, ROWS // 8, forward, 0, unroll=True)

    def stencil(step, carry):
        half, f = step // 2, step % 2
        top = ROWS * 8 * half + NODES * f
        w = [
            [weight[pl.ds(PITCH * 8 * half + 5 * i + j, 8, stride=PITCH), :] * float(QUAD[i, j]) for j in range(5)]
            for i in range(5)
        ]
        p = [[waves_ref[0, pl.ds(top + 5 * i + j, 8, stride=ROWS), :] for j in range(5)] for i in range(5)]
        total = []
        for i in range(5):
            grad = centred(DERIV, p[i])
            total.append(centred(DERIV.T, [w[i][j] * grad[j] for j in range(5)]))
        for j in range(5):
            grad = centred(DERIV, [p[i][j] for i in range(5)])
            part = centred(DERIV.T, [w[i][j] * grad[i] for i in range(5)])
            for i in range(5):
                stress[0, pl.ds(top + 5 * i + j, 8, stride=ROWS), :] = total[i][j] + part[i]
        for i in range(5):
            for j in range(5):
                at = pl.ds(top + 5 * i + j, 8, stride=ROWS)
                stress[1, at, :] = w[i][j] * waves_ref[1, at, :]
        return carry

    lax.fori_loop(0, 4, stencil, 0, unroll=True)
    loads[5].wait()

    def backward(g, carry):
        inv_r = inv[pl.ds(pl.multiple_of(8 * g, 8), 8), :]
        rows = [
            stress[t, pl.ds(pl.multiple_of(ROWS * c + 8 * g, 8), 8), :] for t in range(2) for c in range(16)
        ]
        lhs = jnp.concatenate(rows, axis=0).astype(jnp.bfloat16)
        out = jnp.dot(lhs, back_ref[...], preferred_element_type=jnp.float32)
        terms = []
        for t in range(2):
            v = []
            for c in range(16):
                at = 128 * t + 8 * c
                re, im = out[at : at + 8, :LANES], out[at : at + 8, LANES:]
                if c:
                    cos, sin = twiddle_ref[c : c + 1, :], twiddle_ref[16 + c : 17 + c, :]
                    re, im = re * cos + im * sin, im * cos - re * sin
                v.append((re, im))
            terms.append(gathered(v))
        for a in range(8):
            kept = (lane8 + 128 * a) < limit
            scale = orders[a]
            re = terms[0][a][0] + (scale * terms[1][a][1]) * inv_r
            im = terms[0][a][1] - (scale * terms[1][a][0]) * inv_r
            stiff_ref[pl.ds(128 * g + a, 8, stride=16), :] = jnp.where(kept, re, 0.0)
            stiff_ref[pl.ds(128 * g + 8 + a, 8, stride=16), :] = jnp.where(kept, im, 0.0)
        return carry

    lax.fori_loop(0, ROWS // 8, backward, 0, unroll=True)

    sends = []
    for ids, side, slots, ref, hbm in (
        (blk_ref, 1 - odd, 8, even_ref, even_hbm), (blk_ref, odd, 8, odd_ref, odd_hbm),
        (band_ref, upper, 4, far_ref, far_hbm), (band_ref, 1 - upper, 4, chip_ref, chip_hbm),
    ):
        for k in range(slots):
            at = ids[side, k] * 16
            for f in range(2):
                ref[pl.ds((f * slots + k) * 16, 16), :] = stiff_ref[pl.ds(pl.multiple_of(at + 400 * f, 16), 16), :]
        sends.append(pltpu.make_async_copy(ref, hbm, sems.at[10 + len(sends)]))
        sends[-1].start()
    for load in loads[6:]:
        load.wait()

    @pl.when(first)
    def _():
        finish_locally(limit, scale_ref, waves_ref, stiff_ref, field, late, base_ref, slab, kout)
        store = pltpu.make_async_copy(kout.at[pl.ds(0, 400)], out_hbm, sems.at[9])
        store.start()
        store.wait()

    for send in sends:
        send.wait()


def local_kernel(
    bucket_ref, scale_ref, waves_ref, stiff_ref, field_ref, late_ref, base_in, out_in,
    base_ref, out_hbm, slab, kout, sem,
):
    first, _, _ = device_role()

    @pl.when(first)
    def _():
        base_ref[...] = base_in[...]

    @pl.when(jnp.logical_not(first))
    def _():
        limit = order_limit(bucket_ref[0, 0])
        finish_locally(limit, scale_ref, waves_ref, stiff_ref, field_ref, late_ref, base_ref, slab, kout)
        store = pltpu.make_async_copy(kout.at[pl.ds(0, 400)], out_hbm, sem)
        store.start()
        store.wait()


def join_kernel(
    bucket_ref, count_ref, blk_ref, band_ref, scale_ref, base_ref, odd_ref, even_ref, chip_ref, far_ref, next_ref, last_ref,
    fwd_ref, adj_ref,
):
    limit = order_limit(bucket_ref[0, 0])
    _, odd, upper = device_role()
    slot = lax.broadcasted_iota(jnp.int32, (16, LANES), 0)
    order = lax.broadcasted_iota(jnp.int32, (16, LANES), 1) + 128 * (slot % 8)
    kept = order < limit
    outs = (fwd_ref, adj_ref)
    for f in range(2):
        outs[f][...] = base_ref[pl.ds(400 * f, 400), :]
    for start, ids, side, slots, got in (
        (0, blk_ref, odd, 8, (odd_ref,)), (0, blk_ref, 1 - odd, 8, (even_ref, next_ref)),
        (2, band_ref, 1 - upper, 4, (chip_ref,)), (2, band_ref, upper, 4, (far_ref, last_ref)),
    ):
        count = count_ref[0, start + side]
        for k in range(slots):
            node = ids[side, k]
            take = jnp.logical_and(kept, k < count)
            growth = scale_ref[0, node]
            at = pl.ds(pl.multiple_of(16 * node, 16), 16)
            for f in range(2):
                rows = pl.ds((f * slots + k) * 16, 16)
                step = growth * sum(ref[rows, :] for ref in got)
                outs[f][at, :] = outs[f][at, :] - jnp.where(take, step, 0.0)


def smem():
    return pl.BlockSpec(memory_space=pltpu.SMEM)


def vmem():
    return pl.BlockSpec(memory_space=pltpu.VMEM)


def anywhere():
    return pl.BlockSpec(memory_space=pl.ANY)


def near(*dims):
    return pltpu.VMEM(dims, jnp.float32)


def shape(*dims):
    return jax.ShapeDtypeStruct(dims, jnp.float32)


def swap(value, chosen):
    bands = lax.axis_size("band")
    pairs = [(b * bands + z, c * bands + y) for (b, z), (c, y) in chosen]
    pairs = sorted(pairs + [(target, source) for source, target in pairs])
    return lax.ppermute(value, ("blk", "band"), pairs)


def per_device(
    disp_fwd, prev_fwd, disp_adj, prev_adj, modulus, radius, step_scale, kernel_in, buckets, halo_count,
    blk_nodes, band_nodes,
):
    flat = lambda value: value.reshape(16 * NODES, LANES)
    close = lambda value: pltpu.with_memory_space_constraint(value, pltpu.VMEM)
    table, twiddle = transform_tables()
    bucket, blk, band = buckets.reshape(1, 1), blk_nodes.reshape(2, 8), band_nodes.reshape(2, 4)
    scale = step_scale.reshape(1, NODES)
    blks, bands = lax.axis_size("blk"), lax.axis_size("band")
    f32 = lambda *dims: pltpu.VMEM(dims, jnp.float32)
    stiff, waves, field, late, base, odd, even, chip, far, kernel_out = pl.pallas_call(
        stiffness_kernel,
        out_shape=(
            near(16 * ROWS, LANES), near(2, 16 * ROWS, LANES), near(16 * ROWS, LANES), near(1312, LANES),
            near(800, LANES), shape(256, LANES), shape(256, LANES), shape(128, LANES), shape(128, LANES), shape(400, LANES),
        ),
        in_specs=[smem()] * 5 + [anywhere()] * 9,
        out_specs=(vmem(),) * 5 + (anywhere(),) * 5,
        scratch_shapes=[
            f32(512, LANES), f32(16 * PITCH, LANES), f32(2, 16 * ROWS, LANES), f32(ROWS, LANES), f32(32, LANES),
            pltpu.VMEM((256, 128), jnp.bfloat16), pltpu.VMEM((128, 256), jnp.bfloat16),
            f32(16 * PITCH, LANES), f32(512, LANES), f32(256, LANES), f32(256, LANES), f32(128, LANES), f32(128, LANES),
            pltpu.SemaphoreType.DMA((14,)),
        ],
        cost_estimate=pl.CostEstimate(flops=500_000_000, bytes_accessed=3_000_000, transcendentals=0),
        name="stiffness",
    )(
        bucket, radius.reshape(1, NODES), scale, blk, band, jnp.asarray(twiddle, jnp.float32),
        jnp.asarray(table, jnp.bfloat16), jnp.asarray(table.T, jnp.bfloat16), flat(disp_fwd), flat(disp_adj),
        flat(modulus), flat(prev_fwd), flat(prev_adj), flat(kernel_in),
    )
    far_pairs = [((b, z), (b, z + 1)) for b in range(blks) for z in range(1, bands - 1, 2)]
    blk_pairs = [((b, z), (b + 1, z)) for b in range(blks - 1) for z in range(bands)]
    last = lambda pair: pair[0][0] % RUN == RUN - 1
    even_pairs = [pair for pair in blk_pairs if pair[0][0] % 2 == 0]
    got_even = swap(even, [pair for pair in even_pairs if (pair[0][0] + 1) % RUN != RUN - 1])
    got_far = swap(far, [pair for pair in far_pairs if not last(pair)])
    got_odd = swap(odd, [pair for pair in blk_pairs if pair[0][0] % 2])
    got_next = swap(even, [pair for pair in even_pairs if (pair[0][0] + 1) % RUN == RUN - 1])
    got_last = swap(far, [pair for pair in far_pairs if last(pair)])
    got_chip = swap(chip, [((b, z), (b, z + 1)) for b in range(blks) for z in range(0, bands - 1, 2)])
    base, kernel_out = pl.pallas_call(
        local_kernel,
        out_shape=(near(800, LANES), shape(400, LANES)),
        in_specs=[smem(), smem()] + [vmem()] * 5 + [anywhere()],
        out_specs=(vmem(), anywhere()),
        scratch_shapes=[f32(16 * PITCH, LANES), f32(512, LANES), pltpu.SemaphoreType.DMA],
        input_output_aliases={6: 0, 7: 1},
        cost_estimate=pl.CostEstimate(flops=100_000_000, bytes_accessed=3_000_000, transcendentals=0),
        name="local",
    )(bucket, scale, close(waves), close(stiff), close(field), close(late), close(base), kernel_out)
    next_fwd, next_adj = pl.pallas_call(
        join_kernel,
        out_shape=(shape(400, LANES), shape(400, LANES)),
        in_specs=[smem()] * 5 + [vmem()] * 7,
        out_specs=(vmem(), vmem()),
        cost_estimate=pl.CostEstimate(flops=1_000_000, bytes_accessed=1_500_000, transcendentals=0),
        name="join",
    )(
        bucket, halo_count.reshape(1, 4), blk, band, scale, close(base), close(got_odd), close(got_even),
        close(got_chip), close(got_far), close(got_next), close(got_last),
    )
    return tuple(value.reshape(disp_fwd.shape) for value in (next_fwd, next_adj, kernel_out))


def solution(mesh):
    wide = P("blk", "band", None, None)
    line = P("blk", "band", None)
    in_specs = (wide,) * 5 + (line, line, wide, P("blk", "band"), line, wide, wide)

    return jax.shard_map(per_device, mesh=mesh, in_specs=in_specs, out_specs=(wide, wide, wide), check_vma=False)
```

```python
import math

import jax
import jax.numpy as jnp
import numpy as np
from jax import lax
from jax.experimental import pallas as pl
from jax.experimental.pallas import tpu as pltpu
from jax.sharding import PartitionSpec as P


NODES = 25
ROWS = 56
PITCH = 40
RUN = 12
EARLY_EVEN, EARLY_FAR = 5, 7
LANES = 128


def gll_tables():
    inner_root = math.sqrt(3.0 / 7.0)
    points = np.array([-1.0, -inner_root, 0.0, inner_root, 1.0])
    weights = np.array([0.1, 49.0 / 90.0, 32.0 / 45.0, 49.0 / 90.0, 0.1])
    legendre = (35.0 * points**4 - 30.0 * points**2 + 3.0) / 8.0
    derivative = np.zeros((5, 5))
    for target in range(5):
        for source in range(5):
            if target != source:
                derivative[target, source] = (
                    legendre[target] / legendre[source] / (points[target] - points[source])
                )
    derivative[0, 0] = -5.0
    derivative[4, 4] = 5.0
    return derivative, np.outer(weights, weights)


DERIV, QUAD = gll_tables()


def transform_tables():
    column = np.arange(2 * LANES)
    lane = column % LANES
    sample = 16 * (8 * (column // LANES) + lane % 8) + lane // 8
    angle = 2.0 * np.pi * ((np.arange(256)[:, None] * sample[None, :]) % 256) / 256.0
    table = np.concatenate([np.cos(angle), -np.sin(angle)], axis=0) / 32.0
    turn = (2.0 * np.pi * np.arange(8)[:, None] * column[None, :] / 2048.0).reshape(16, LANES)
    twiddle = np.concatenate([np.cos(turn), np.sin(turn)], axis=0)
    return table, twiddle


def times_root(z, eighth, sign):
    re, im = z
    root = math.sqrt(0.5)
    if eighth == 0:
        return z
    if eighth == 1:
        return ((re - im) * root, (re + im) * root) if sign > 0 else ((re + im) * root, (im - re) * root)
    if eighth == 2:
        return (-im, re) if sign > 0 else (im, -re)
    return ((-re - im) * root, (re - im) * root) if sign > 0 else ((im - re) * root, (-re - im) * root)


def plus(x, y):
    return (x[0] + y[0], x[1] + y[1])


def minus(x, y):
    return (x[0] - y[0], x[1] - y[1])


def plus_turned(x, y, sign):
    return (x[0] - y[1], x[1] + y[0]) if sign > 0 else (x[0] + y[1], x[1] - y[0])


def dft4(a, b, c, d, sign):
    s, t, u, v = plus(a, c), minus(a, c), plus(b, d), minus(b, d)
    return [plus(s, u), plus_turned(t, v, sign), minus(s, u), plus_turned(t, v, -sign)]


def spread(z):
    even = dft4(*z, 1)
    odd = dft4(*(times_root(term, m, 1) for m, term in enumerate(z)), 1)
    return [(even, odd)[k % 2][k // 2] for k in range(8)]


def gathered(v):
    even = dft4(*v[0::2], -1)
    odd = dft4(*v[1::2], -1)
    return [plus(even[m], times_root(odd[m], m, -1)) for m in range(4)]


def centred(table, p):
    e0, o0, e1, o1, c = p[0] + p[4], p[0] - p[4], p[1] + p[3], p[1] - p[3], p[2]
    out = [None] * 5
    for i in range(2):
        t = table[i]
        odd = o0 * float(0.5 * (t[0] - t[4])) + o1 * float(0.5 * (t[1] - t[3]))
        even = e0 * float(0.5 * (t[0] + t[4])) + e1 * float(0.5 * (t[1] + t[3])) + c * float(t[2])
        out[i], out[4 - i] = odd + even, odd - even
    out[2] = o0 * float(table[2, 0]) + o1 * float(table[2, 1])
    return out


def swap_blocks(x):
    lane = lax.broadcasted_iota(jnp.int32, x[0].shape, 1)
    for bit in (4, 2, 1):
        clear = (lane & bit) == 0
        for s in range(8):
            if s & bit:
                continue
            a, b = x[s], x[s | bit]
            x[s] = jnp.where(clear, a, pltpu.roll(b, bit, 1))
            x[s | bit] = jnp.where(clear, pltpu.roll(a, LANES - bit, 1), b)
    return x


def order_limit(bucket):
    return jnp.where(bucket == 0, 16, jnp.where(bucket == 1, 64, jnp.where(bucket == 2, 256, 1024)))


def device_role():
    blk, band = lax.axis_index("blk"), lax.axis_index("band")
    return lax.rem(blk, RUN) == 0, lax.rem(blk, 2), lax.rem(band, 2)


def finish_locally(limit, scale_ref, waves_ref, stiff_ref, field_ref, late_ref, base_ref, slab, kout):
    slot = lax.broadcasted_iota(jnp.int32, (16, LANES), 0)
    order = lax.broadcasted_iota(jnp.int32, (16, LANES), 1) + 128 * (slot % 8)
    kept = order < limit

    def update(n, carry):
        growth = scale_ref[0, n]
        for f in range(2):
            rows = pl.ds(pl.multiple_of(16 * n + 400 * f, 16), 16)
            value = 2.0 * field_ref[rows, :] - late_ref[rows, :] - growth * stiff_ref[rows, :]
            base_ref[rows, :] = jnp.where(kept, value, 0.0)
        return carry

    lax.fori_loop(0, NODES, update, 0, unroll=5)

    for u in range(2):
        p = [
            [[waves_ref[0, u, pl.ds(NODES * f + 5 * i + j, 8, stride=ROWS), :] for j in range(5)] for i in range(5)]
            for f in range(2)
        ]
        total = [
            [
                waves_ref[1, u, pl.ds(5 * i + j, 8, stride=ROWS), :]
                * waves_ref[1, u, pl.ds(NODES + 5 * i + j, 8, stride=ROWS), :]
                for j in range(5)
            ]
            for i in range(5)
        ]
        for i in range(5):
            fwd, adj = centred(DERIV, p[0][i]), centred(DERIV, p[1][i])
            for j in range(5):
                total[i][j] = total[i][j] + fwd[j] * adj[j]
        for j in range(5):
            fwd, adj = (centred(DERIV, [p[f][i][j] for i in range(5)]) for f in range(2))
            for i in range(5):
                slab[u, pl.ds(5 * i + j, 8, stride=PITCH), :] = (total[i][j] + fwd[i] * adj[i]) * float(QUAD[i, j])

    for g in range(4):
        for u in range(2):
            x = swap_blocks([slab[u, pl.ds(PITCH * c + 8 * g, 8), :] for c in range(8)])
            for s in range(8):
                at = 128 * g + 8 * u + s
                kout[pl.ds(at, 8, stride=16), :] = late_ref[pl.ds(800 + at, 8, stride=16), :] - x[s]


SCALARS = (
    pltpu.SMEM((1, 1), jnp.int32), pltpu.SMEM((1, NODES), jnp.float32), pltpu.SMEM((1, NODES), jnp.float32),
    pltpu.SMEM((2, 8), jnp.int32), pltpu.SMEM((2, 4), jnp.int32), pltpu.SMEM((1, 4), jnp.int32),
)


def scalar_loads(sources, targets, sems):
    return [
        pltpu.make_async_copy(source, target, sems.at[i])
        for i, (source, target) in enumerate(zip(sources, targets))
    ]


def stiffness_kernel(
    bucket_hbm, radius_hbm, scale_hbm, blk_hbm, band_hbm, count_hbm, twiddle_hbm, table_hbm, back_hbm, fwd_hbm, adj_hbm, mod_hbm,
    prev_fwd_hbm, prev_adj_hbm, kernel_hbm,
    stiff_ref, waves_ref, field, late, base_ref, odd_hbm, even_hbm, chip_hbm, far_hbm, out_hbm, table_out, growth_out,
    mod, weight, stress, inv, twiddle_ref, table_ref, back_ref, slab, kout, odd_ref, even_ref, chip_ref, far_ref,
    bucket_ref, radius_ref, scale_ref, blk_ref, band_ref, count_ref, sems, scalar_sems,
):
    scalars = scalar_loads(
        (radius_hbm, bucket_hbm, scale_hbm, blk_hbm, band_hbm, count_hbm),
        (radius_ref, bucket_ref, scale_ref, blk_ref, band_ref, count_ref),
        scalar_sems,
    )
    loads = [
        pltpu.make_async_copy(source, target, sems.at[i])
        for i, (source, target) in enumerate((
            (fwd_hbm, field.at[pl.ds(0, 400)]), (adj_hbm, field.at[pl.ds(400, 400)]), (twiddle_hbm, twiddle_ref),
            (table_hbm, table_ref), (mod_hbm, mod.at[pl.ds(0, 400)]), (back_hbm, back_ref),
            (prev_fwd_hbm, late.at[pl.ds(0, 400)]), (prev_adj_hbm, late.at[pl.ds(400, 400)]),
            (kernel_hbm, late.at[pl.ds(800, 400)]),
        ))
    ]
    for load in loads[:2]:
        load.start()
    for load in scalars:
        load.start()
    for load in loads[2:6]:
        load.start()
    for load in scalars:
        load.wait()
    limit = order_limit(bucket_ref[0, 0])
    first, odd, upper = device_role()
    lane8 = lax.broadcasted_iota(jnp.int32, (8, LANES), 1)
    orders = [(lane8 + 128 * a).astype(jnp.float32) for a in range(8)]

    inv[pl.ds(ROWS - 8, 8), :] = jnp.ones((8, LANES), jnp.float32)
    for n in range(NODES):
        line = jnp.full((1, LANES), radius_ref[0, n], jnp.float32)
        inv[pl.ds(n, 1), :] = line
        inv[pl.ds(NODES + n, 1), :] = line
    inv[...] = 1.0 / inv[...]
    for load in loads[:4]:
        load.wait()
    for load in loads[6:]:
        load.start()

    def forward(g, carry):
        inv_r = inv[pl.ds(pl.multiple_of(8 * g, 8), 8), :]
        base = 128 * g
        u, w = [], []
        for a in range(8):
            kept = (lane8 + 128 * a) < limit
            re = jnp.where(kept, field[pl.ds(base + a, 8, stride=16), :], 0.0)
            im = jnp.where(kept, field[pl.ds(base + 8 + a, 8, stride=16), :], 0.0)
            scale = orders[a]
            w.append((-(scale * im) * inv_r, (scale * re) * inv_r))
            u.append((re, im))
        parts = [[], [], [], []]
        for z in (u, w):
            z = [tuple(part.astype(jnp.bfloat16).astype(jnp.float32) for part in term) for term in z]
            for half in range(2):
                for c, (re, im) in enumerate(spread(z[half::2])):
                    if c:
                        at = 2 * c + half
                        cos, sin = twiddle_ref[at : at + 1, :], twiddle_ref[16 + at : 17 + at, :]
                        re, im = re * cos - im * sin, re * sin + im * cos
                    parts[half].append(re)
                    parts[2 + half].append(im)
        lhs = jnp.concatenate([jnp.concatenate(part, axis=0) for part in parts], axis=1)
        out = jnp.dot(lhs.astype(jnp.bfloat16), table_ref[...], preferred_element_type=jnp.float32)
        for t in range(2):
            for c in range(8):
                for half in range(2):
                    at = pl.multiple_of(ROWS * c + 8 * g, 8)
                    waves_ref[t, half, pl.ds(at, 8), :] = out[
                        64 * t + 8 * c : 64 * t + 8 * c + 8, LANES * half : LANES * (half + 1)
                    ]
        return carry

    loads[4].wait()

    def reorder(g, carry):
        for half in range(2):
            x = swap_blocks([mod[pl.ds(128 * g + 8 * half + s, 8, stride=16), :] for s in range(8)])
            for c in range(8):
                weight[half, pl.ds(pl.multiple_of(PITCH * c + 8 * g, 8), 8), :] = x[c]
        return carry

    lax.fori_loop(0, 4, lambda g, carry: reorder(g, forward(g, carry)), 0, unroll=True)
    lax.fori_loop(4, ROWS // 8, forward, 0, unroll=True)

    for u, f in ((0, 0), (0, 1), (1, 0), (1, 1)):
        top = NODES * f
        w = [
            [weight[u, pl.ds(5 * i + j, 8, stride=PITCH), :] * float(QUAD[i, j]) for j in range(5)] for i in range(5)
        ]
        p = [[waves_ref[0, u, pl.ds(top + 5 * i + j, 8, stride=ROWS), :] for j in range(5)] for i in range(5)]
        total = []
        for i in range(5):
            grad = centred(DERIV, p[i])
            total.append(centred(DERIV.T, [w[i][j] * grad[j] for j in range(5)]))
        for j in range(5):
            grad = centred(DERIV, [p[i][j] for i in range(5)])
            part = centred(DERIV.T, [w[i][j] * grad[i] for i in range(5)])
            for i in range(5):
                stress[0, u, pl.ds(top + 5 * i + j, 8, stride=ROWS), :] = total[i][j] + part[i]
        for i in range(5):
            for j in range(5):
                at = pl.ds(top + 5 * i + j, 8, stride=ROWS)
                stress[1, u, at, :] = w[i][j] * waves_ref[1, u, at, :]
    loads[5].wait()

    def backward(g, carry):
        inv_r = inv[pl.ds(pl.multiple_of(8 * g, 8), 8), :]
        at = [pl.ds(pl.multiple_of(ROWS * c + 8 * g, 8), 8) for c in range(8)]
        lhs = jnp.concatenate(
            [
                jnp.concatenate([stress[t, u, at[c], :] for t in range(2) for c in range(8)], axis=0)
                for u in range(2)
            ],
            axis=1,
        )
        out = jnp.dot(lhs.astype(jnp.bfloat16), back_ref[...], preferred_element_type=jnp.float32)
        terms = []
        for t in range(2):
            halves = []
            for half in range(2):
                v = []
                for c in range(8):
                    rows = out[64 * t + 8 * c : 64 * t + 8 * c + 8]
                    re = rows[:, LANES * half : LANES * (half + 1)]
                    im = rows[:, LANES * (2 + half) : LANES * (3 + half)]
                    if c:
                        k = 2 * c + half
                        cos, sin = twiddle_ref[k : k + 1, :], twiddle_ref[16 + k : 17 + k, :]
                        re, im = re * cos + im * sin, im * cos - re * sin
                    v.append((re, im))
                halves.append(gathered(v))
            terms.append([halves[a % 2][a // 2] for a in range(8)])
        for a in range(8):
            kept = (lane8 + 128 * a) < limit
            scale = orders[a]
            re = terms[0][a][0] + (scale * terms[1][a][1]) * inv_r
            im = terms[0][a][1] - (scale * terms[1][a][0]) * inv_r
            stiff_ref[pl.ds(128 * g + a, 8, stride=16), :] = jnp.where(kept, re, 0.0)
            stiff_ref[pl.ds(128 * g + 8 + a, 8, stride=16), :] = jnp.where(kept, im, 0.0)
        return carry

    lax.fori_loop(0, ROWS // 8, backward, 0, unroll=True)

    table_out[0, 0] = limit
    for side in range(2):
        table_out[0, 1 + side] = count_ref[0, side]
        table_out[0, 3 + side] = count_ref[0, 2 + side]
        for k in range(8):
            table_out[0, 8 + 8 * side + k] = blk_ref[side, k]
        for k in range(4):
            table_out[0, 24 + 4 * side + k] = band_ref[side, k]
    for n in range(NODES):
        growth_out[0, n] = scale_ref[0, n]
    sends = []
    for ids, side, slots, ref, hbm in (
        (blk_ref, 1 - odd, 8, even_ref, even_hbm), (blk_ref, odd, 8, odd_ref, odd_hbm),
        (band_ref, upper, 4, far_ref, far_hbm), (band_ref, 1 - upper, 4, chip_ref, chip_hbm),
    ):
        for k in range(slots):
            at = ids[side, k] * 16
            for f in range(2):
                ref[pl.ds((f * slots + k) * 16, 16), :] = stiff_ref[pl.ds(pl.multiple_of(at + 400 * f, 16), 16), :]
        sends.append(pltpu.make_async_copy(ref, hbm, sems.at[10 + len(sends)]))
        sends[-1].start()
    for load in loads[6:]:
        load.wait()

    @pl.when(first)
    def _():
        finish_locally(limit, scale_ref, waves_ref, stiff_ref, field, late, base_ref, slab, kout)
        store = pltpu.make_async_copy(kout.at[pl.ds(0, 400)], out_hbm, sems.at[9])
        store.start()
        store.wait()

    for send in sends:
        send.wait()


def local_kernel(
    numbers_ref, scale_ref, waves_ref, stiff_ref, field_ref, late_ref, base_in, out_in,
    base_ref, out_hbm, slab, kout, sem,
):
    first, _, _ = device_role()

    @pl.when(first)
    def _():
        base_ref[...] = base_in[...]

    @pl.when(jnp.logical_not(first))
    def _():
        limit = numbers_ref[0, 0]
        finish_locally(limit, scale_ref, waves_ref, stiff_ref, field_ref, late_ref, base_ref, slab, kout)
        store = pltpu.make_async_copy(kout.at[pl.ds(0, 400)], out_hbm, sem)
        store.start()
        store.wait()


def join_kernel(
    numbers_ref, scale_ref, base_ref, odd_ref, even_ref, chip_ref, far_ref, next_ref, last_ref,
    fwd_hbm, adj_hbm, total, sems,
):
    _, odd, upper = device_role()
    slot = lax.broadcasted_iota(jnp.int32, (16, LANES), 0)
    order = lax.broadcasted_iota(jnp.int32, (16, LANES), 1) + 128 * (slot % 8)
    kept = order < numbers_ref[0, 0]
    total[...] = base_ref[...]
    stores = []
    for f, out_hbm in enumerate((fwd_hbm, adj_hbm)):
        for start, ids, side, slots, got in (
            (1, 8, odd, 8, (odd_ref,)), (1, 8, 1 - odd, 8, (even_ref, next_ref)),
            (3, 24, 1 - upper, 4, (chip_ref,)), (3, 24, upper, 4, (far_ref, last_ref)),
        ):
            count = numbers_ref[0, start + side]
            for k in range(slots):
                node = numbers_ref[0, ids + slots * side + k]
                take = jnp.logical_and(kept, k < count)
                at = pl.ds(pl.multiple_of(16 * node + 400 * f, 16), 16)
                rows = pl.ds((f * slots + k) * 16, 16)
                step = scale_ref[0, node] * sum(ref[rows, :] for ref in got)
                total[at, :] = base_ref[at, :] - jnp.where(take, step, 0.0)
        stores.append(pltpu.make_async_copy(total.at[pl.ds(400 * f, 400)], out_hbm, sems.at[f]))
        stores[-1].start()
    for store in stores:
        store.wait()


def smem():
    return pl.BlockSpec(memory_space=pltpu.SMEM)


def vmem():
    return pl.BlockSpec(memory_space=pltpu.VMEM)


def anywhere():
    return pl.BlockSpec(memory_space=pl.ANY)


def near(*dims):
    return pltpu.VMEM(dims, jnp.float32)


def shape(*dims):
    return jax.ShapeDtypeStruct(dims, jnp.float32)


def swap(value, chosen):
    bands = lax.axis_size("band")
    pairs = [(b * bands + z, c * bands + y) for (b, z), (c, y) in chosen]
    pairs = sorted(pairs + [(target, source) for source, target in pairs])
    return lax.ppermute(value, ("blk", "band"), pairs)


def per_device(
    disp_fwd, prev_fwd, disp_adj, prev_adj, modulus, radius, step_scale, kernel_in, buckets, halo_count,
    blk_nodes, band_nodes,
):
    flat = lambda value: value.reshape(16 * NODES, LANES)
    inside = lambda value: pltpu.with_memory_space_constraint(value, pltpu.SMEM)
    close = lambda value: pltpu.with_memory_space_constraint(value, pltpu.VMEM)
    table, twiddle = transform_tables()
    bucket, blk, band = buckets.reshape(1, 1), blk_nodes.reshape(2, 8), band_nodes.reshape(2, 4)
    scale = step_scale.reshape(1, NODES)
    blks, bands = lax.axis_size("blk"), lax.axis_size("band")
    f32 = lambda *dims: pltpu.VMEM(dims, jnp.float32)
    stiff, waves, field, late, base, odd, even, chip, far, kernel_out, numbers, growth = pl.pallas_call(
        stiffness_kernel,
        out_shape=(
            near(16 * ROWS, LANES), near(2, 2, 8 * ROWS, LANES), near(16 * ROWS, LANES), near(1312, LANES),
            near(800, LANES), shape(256, LANES), shape(256, LANES), shape(128, LANES), shape(128, LANES), shape(400, LANES),
            pltpu.SMEM((1, 32), jnp.int32), pltpu.SMEM((1, NODES), jnp.float32),
        ),
        in_specs=[anywhere()] * 15,
        out_specs=(vmem(),) * 5 + (anywhere(),) * 5 + (smem(), smem()),
        scratch_shapes=[
            f32(512, LANES), f32(2, 8 * PITCH, LANES), f32(2, 2, 8 * ROWS, LANES), f32(ROWS, LANES), f32(32, LANES),
            pltpu.VMEM((512, 256), jnp.bfloat16), pltpu.VMEM((256, 512), jnp.bfloat16),
            f32(2, 8 * PITCH, LANES), f32(512, LANES), f32(256, LANES), f32(256, LANES), f32(128, LANES), f32(128, LANES),
            *SCALARS, pltpu.SemaphoreType.DMA((14,)), pltpu.SemaphoreType.DMA((6,)),
        ],
        cost_estimate=pl.CostEstimate(flops=500_000_000, bytes_accessed=3_000_000, transcendentals=0),
        name="stiffness",
    )(
        bucket, radius.reshape(1, NODES), scale, blk, band, halo_count.reshape(1, 4), jnp.asarray(twiddle, jnp.float32),
        jnp.asarray(table, jnp.bfloat16), jnp.asarray(table.T, jnp.bfloat16), flat(disp_fwd), flat(disp_adj),
        flat(modulus), flat(prev_fwd), flat(prev_adj), flat(kernel_in),
    )
    far_pairs = [((b, z), (b, z + 1)) for b in range(blks) for z in range(1, bands - 1, 2)]
    blk_pairs = [((b, z), (b + 1, z)) for b in range(blks - 1) for z in range(bands)]
    place = lambda pair: pair[0][0] % RUN
    even_pairs = [pair for pair in blk_pairs if pair[0][0] % 2 == 0]
    got_even = swap(even, [pair for pair in even_pairs if place(pair) < EARLY_EVEN])
    got_far = swap(far, [pair for pair in far_pairs if place(pair) < EARLY_FAR])
    got_odd = swap(odd, [pair for pair in blk_pairs if pair[0][0] % 2])
    got_chip = swap(chip, [((b, z), (b, z + 1)) for b in range(blks) for z in range(0, bands - 1, 2)])
    got_last = swap(far, [pair for pair in far_pairs if place(pair) >= EARLY_FAR])
    got_next = swap(even, [pair for pair in even_pairs if place(pair) >= EARLY_EVEN])
    base, kernel_out = pl.pallas_call(
        local_kernel,
        out_shape=(near(800, LANES), shape(400, LANES)),
        in_specs=[smem()] * 2 + [vmem()] * 5 + [anywhere()],
        out_specs=(vmem(), anywhere()),
        scratch_shapes=[f32(2, 8 * PITCH, LANES), f32(512, LANES), pltpu.SemaphoreType.DMA],
        input_output_aliases={6: 0, 7: 1},
        cost_estimate=pl.CostEstimate(flops=100_000_000, bytes_accessed=3_000_000, transcendentals=0),
        name="local",
    )(inside(numbers), inside(growth), close(waves), close(stiff), close(field), close(late), close(base), kernel_out)
    next_fwd, next_adj = pl.pallas_call(
        join_kernel,
        out_shape=(shape(400, LANES), shape(400, LANES)),
        in_specs=[smem()] * 2 + [vmem()] * 7,
        out_specs=(anywhere(), anywhere()),
        scratch_shapes=[f32(800, LANES), pltpu.SemaphoreType.DMA((2,))],
        cost_estimate=pl.CostEstimate(flops=1_000_000, bytes_accessed=1_500_000, transcendentals=0),
        name="join",
    )(
        inside(numbers), inside(growth), close(base), close(got_odd), close(got_even),
        close(got_chip), close(got_far), close(got_next), close(got_last),
    )
    return tuple(value.reshape(disp_fwd.shape) for value in (next_fwd, next_adj, kernel_out))


def solution(mesh):
    wide = P("blk", "band", None, None)
    line = P("blk", "band", None)
    in_specs = (wide,) * 5 + (line, line, wide, P("blk", "band"), line, wide, wide)

    return jax.shard_map(per_device, mesh=mesh, in_specs=in_specs, out_specs=(wide, wide, wide), check_vma=False)
```

```python
import math

import jax
import jax.numpy as jnp
import numpy as np
from jax import lax
from jax.experimental import pallas as pl
from jax.experimental.pallas import tpu as pltpu
from jax.sharding import PartitionSpec as P


NODES = 25
ROWS = 56
PITCH = 40
RUN = 12
EARLY_EVEN, EARLY_FAR = 5, 7
LANES = 128


def gll_tables():
    inner_root = math.sqrt(3.0 / 7.0)
    points = np.array([-1.0, -inner_root, 0.0, inner_root, 1.0])
    weights = np.array([0.1, 49.0 / 90.0, 32.0 / 45.0, 49.0 / 90.0, 0.1])
    legendre = (35.0 * points**4 - 30.0 * points**2 + 3.0) / 8.0
    derivative = np.zeros((5, 5))
    for target in range(5):
        for source in range(5):
            if target != source:
                derivative[target, source] = (
                    legendre[target] / legendre[source] / (points[target] - points[source])
                )
    derivative[0, 0] = -5.0
    derivative[4, 4] = 5.0
    return derivative, np.outer(weights, weights)


DERIV, QUAD = gll_tables()


def transform_tables():
    column = np.arange(2 * LANES)
    lane = column % LANES
    sample = 16 * (8 * (column // LANES) + lane % 8) + lane // 8
    angle = 2.0 * np.pi * ((np.arange(256)[:, None] * sample[None, :]) % 256) / 256.0
    table = np.concatenate([np.cos(angle), -np.sin(angle)], axis=0) / 32.0
    turn = (2.0 * np.pi * np.arange(8)[:, None] * column[None, :] / 2048.0).reshape(16, LANES)
    twiddle = np.concatenate([np.cos(turn), np.sin(turn)], axis=0)
    return table, twiddle


def times_root(z, eighth, sign):
    re, im = z
    root = math.sqrt(0.5)
    if eighth == 0:
        return z
    if eighth == 1:
        return ((re - im) * root, (re + im) * root) if sign > 0 else ((re + im) * root, (im - re) * root)
    if eighth == 2:
        return (-im, re) if sign > 0 else (im, -re)
    return ((-re - im) * root, (re - im) * root) if sign > 0 else ((im - re) * root, (-re - im) * root)


def plus(x, y):
    return (x[0] + y[0], x[1] + y[1])


def minus(x, y):
    return (x[0] - y[0], x[1] - y[1])


def plus_turned(x, y, sign):
    return (x[0] - y[1], x[1] + y[0]) if sign > 0 else (x[0] + y[1], x[1] - y[0])


def dft4(a, b, c, d, sign):
    s, t, u, v = plus(a, c), minus(a, c), plus(b, d), minus(b, d)
    return [plus(s, u), plus_turned(t, v, sign), minus(s, u), plus_turned(t, v, -sign)]


def spread(z):
    even = dft4(*z, 1)
    odd = dft4(*(times_root(term, m, 1) for m, term in enumerate(z)), 1)
    return [(even, odd)[k % 2][k // 2] for k in range(8)]


def gathered(v):
    even = dft4(*v[0::2], -1)
    odd = dft4(*v[1::2], -1)
    return [plus(even[m], times_root(odd[m], m, -1)) for m in range(4)]


def centred(table, p):
    e0, o0, e1, o1, c = p[0] + p[4], p[0] - p[4], p[1] + p[3], p[1] - p[3], p[2]
    out = [None] * 5
    for i in range(2):
        t = table[i]
        odd = o0 * float(0.5 * (t[0] - t[4])) + o1 * float(0.5 * (t[1] - t[3]))
        even = e0 * float(0.5 * (t[0] + t[4])) + e1 * float(0.5 * (t[1] + t[3])) + c * float(t[2])
        out[i], out[4 - i] = odd + even, odd - even
    out[2] = o0 * float(table[2, 0]) + o1 * float(table[2, 1])
    return out


def swap_blocks(x):
    lane = lax.broadcasted_iota(jnp.int32, x[0].shape, 1)
    for bit in (4, 2, 1):
        clear = (lane & bit) == 0
        for s in range(8):
            if s & bit:
                continue
            a, b = x[s], x[s | bit]
            x[s] = jnp.where(clear, a, pltpu.roll(b, bit, 1))
            x[s | bit] = jnp.where(clear, pltpu.roll(a, LANES - bit, 1), b)
    return x


def order_limit(bucket):
    return jnp.where(bucket == 0, 16, jnp.where(bucket == 1, 64, jnp.where(bucket == 2, 256, 1024)))


def device_role():
    blk, band = lax.axis_index("blk"), lax.axis_index("band")
    return lax.rem(blk, RUN) == 0, lax.rem(blk, 2), lax.rem(band, 2)


def finish_locally(limit, scale_ref, waves_ref, stiff_ref, field_ref, late_ref, base_ref, slab, kout):
    slot = lax.broadcasted_iota(jnp.int32, (16, LANES), 0)
    order = lax.broadcasted_iota(jnp.int32, (16, LANES), 1) + 128 * (slot % 8)
    kept = order < limit

    def update(n, carry):
        growth = scale_ref[0, n]
        for f in range(2):
            rows = pl.ds(pl.multiple_of(16 * n + 400 * f, 16), 16)
            value = 2.0 * field_ref[rows, :] - late_ref[rows, :] - growth * stiff_ref[rows, :]
            base_ref[rows, :] = jnp.where(kept, value, 0.0)
        return carry

    lax.fori_loop(0, NODES, update, 0, unroll=5)

    for u in range(2):
        p = [
            [[waves_ref[0, u, pl.ds(NODES * f + 5 * i + j, 8, stride=ROWS), :] for j in range(5)] for i in range(5)]
            for f in range(2)
        ]
        total = [
            [
                waves_ref[1, u, pl.ds(5 * i + j, 8, stride=ROWS), :]
                * waves_ref[1, u, pl.ds(NODES + 5 * i + j, 8, stride=ROWS), :]
                for j in range(5)
            ]
            for i in range(5)
        ]
        for i in range(5):
            fwd, adj = centred(DERIV, p[0][i]), centred(DERIV, p[1][i])
            for j in range(5):
                total[i][j] = total[i][j] + fwd[j] * adj[j]
        for j in range(5):
            fwd, adj = (centred(DERIV, [p[f][i][j] for i in range(5)]) for f in range(2))
            for i in range(5):
                slab[u, pl.ds(5 * i + j, 8, stride=PITCH), :] = (total[i][j] + fwd[i] * adj[i]) * float(QUAD[i, j])

    for g in range(4):
        for u in range(2):
            x = swap_blocks([slab[u, pl.ds(PITCH * c + 8 * g, 8), :] for c in range(8)])
            for s in range(8):
                at = 128 * g + 8 * u + s
                kout[pl.ds(at, 8, stride=16), :] = late_ref[pl.ds(800 + at, 8, stride=16), :] - x[s]


SCALARS = (
    pltpu.SMEM((1, 1), jnp.int32), pltpu.SMEM((1, NODES), jnp.float32), pltpu.SMEM((1, NODES), jnp.float32),
    pltpu.SMEM((2, 8), jnp.int32), pltpu.SMEM((2, 4), jnp.int32), pltpu.SMEM((1, 4), jnp.int32),
)


def scalar_loads(sources, targets, sems):
    return [
        pltpu.make_async_copy(source, target, sems.at[i])
        for i, (source, target) in enumerate(zip(sources, targets))
    ]


def stiffness_kernel(
    bucket_hbm, radius_hbm, scale_hbm, blk_hbm, band_hbm, count_hbm, twiddle_hbm, table_hbm, back_hbm, fwd_hbm, adj_hbm, mod_hbm,
    prev_fwd_hbm, prev_adj_hbm, kernel_hbm,
    stiff_ref, waves_ref, field, late, base_ref, odd_hbm, even_hbm, chip_hbm, far_hbm, out_hbm, table_out, growth_out,
    mod, weight, stress, inv, twiddle_ref, table_ref, back_ref, slab, kout, odd_ref, even_ref, chip_ref, far_ref,
    bucket_ref, radius_ref, scale_ref, blk_ref, band_ref, count_ref, sems, scalar_sems,
):
    scalars = scalar_loads(
        (radius_hbm, bucket_hbm, scale_hbm, blk_hbm, band_hbm, count_hbm),
        (radius_ref, bucket_ref, scale_ref, blk_ref, band_ref, count_ref),
        scalar_sems,
    )
    loads = [
        pltpu.make_async_copy(source, target, sems.at[i])
        for i, (source, target) in enumerate((
            (fwd_hbm.at[pl.ds(0, 128)], field.at[pl.ds(0, 128)]), (twiddle_hbm, twiddle_ref), (table_hbm, table_ref),
            (fwd_hbm.at[pl.ds(128, 272)], field.at[pl.ds(128, 272)]), (adj_hbm, field.at[pl.ds(400, 400)]),
            (mod_hbm, mod.at[pl.ds(0, 400)]), (back_hbm, back_ref),
            (prev_fwd_hbm, late.at[pl.ds(0, 400)]), (prev_adj_hbm, late.at[pl.ds(400, 400)]),
            (kernel_hbm, late.at[pl.ds(800, 400)]),
        ))
    ]
    loads[0].start()
    for load in scalars:
        load.start()
    for load in loads[1:7]:
        load.start()
    for load in scalars:
        load.wait()
    limit = order_limit(bucket_ref[0, 0])
    first, odd, upper = device_role()
    lane8 = lax.broadcasted_iota(jnp.int32, (8, LANES), 1)
    orders = [(lane8 + 128 * a).astype(jnp.float32) for a in range(8)]

    inv[pl.ds(ROWS - 8, 8), :] = jnp.ones((8, LANES), jnp.float32)
    for n in range(NODES):
        line = jnp.full((1, LANES), radius_ref[0, n], jnp.float32)
        inv[pl.ds(n, 1), :] = line
        inv[pl.ds(NODES + n, 1), :] = line
    inv[...] = 1.0 / inv[...]
    for load in loads[:2]:
        load.wait()

    def forward(g, carry):
        inv_r = inv[pl.ds(8 * g, 8), :]
        base = 128 * g
        u, w = [], []
        for a in range(8):
            kept = (lane8 + 128 * a) < limit
            re = jnp.where(kept, field[pl.ds(base + a, 8, stride=16), :], 0.0)
            im = jnp.where(kept, field[pl.ds(base + 8 + a, 8, stride=16), :], 0.0)
            scale = orders[a]
            w.append((-(scale * im) * inv_r, (scale * re) * inv_r))
            u.append((re, im))
        parts = [[], [], [], []]
        for z in (u, w):
            z = [tuple(part.astype(jnp.bfloat16).astype(jnp.float32) for part in term) for term in z]
            for half in range(2):
                for c, (re, im) in enumerate(spread(z[half::2])):
                    if c:
                        at = 2 * c + half
                        cos, sin = twiddle_ref[at : at + 1, :], twiddle_ref[16 + at : 17 + at, :]
                        re, im = re * cos - im * sin, re * sin + im * cos
                    parts[half].append(re)
                    parts[2 + half].append(im)
        lhs = jnp.concatenate([jnp.concatenate(part, axis=0) for part in parts], axis=1)
        if g == 0:
            loads[2].wait()
        out = jnp.dot(lhs.astype(jnp.bfloat16), table_ref[...], preferred_element_type=jnp.float32)
        for t in range(2):
            for c in range(8):
                for half in range(2):
                    at = ROWS * c + 8 * g
                    waves_ref[t, half, pl.ds(at, 8), :] = out[
                        64 * t + 8 * c : 64 * t + 8 * c + 8, LANES * half : LANES * (half + 1)
                    ]
        return carry

    def reorder(g, carry):
        for half in range(2):
            x = swap_blocks([mod[pl.ds(128 * g + 8 * half + s, 8, stride=16), :] for s in range(8)])
            for c in range(8):
                weight[half, pl.ds(PITCH * c + 8 * g, 8), :] = x[c]
        return carry

    for g in range(ROWS // 8):
        if g == 1:
            loads[3].wait()
        if g == 3:
            loads[4].wait()
            loads[5].wait()
            for load in loads[7:]:
                load.start()
        forward(g, 0)
        if g >= 3:
            reorder(g - 3, 0)

    for u, f in ((0, 0), (0, 1), (1, 0), (1, 1)):
        top = NODES * f
        if f == 0:
            w = [
                [weight[u, pl.ds(5 * i + j, 8, stride=PITCH), :] * float(QUAD[i, j]) for j in range(5)]
                for i in range(5)
            ]
        p = [[waves_ref[0, u, pl.ds(top + 5 * i + j, 8, stride=ROWS), :] for j in range(5)] for i in range(5)]
        total = []
        for i in range(5):
            grad = centred(DERIV, p[i])
            total.append(centred(DERIV.T, [w[i][j] * grad[j] for j in range(5)]))
        for j in range(5):
            grad = centred(DERIV, [p[i][j] for i in range(5)])
            part = centred(DERIV.T, [w[i][j] * grad[i] for i in range(5)])
            for i in range(5):
                stress[0, u, pl.ds(top + 5 * i + j, 8, stride=ROWS), :] = total[i][j] + part[i]
        for i in range(5):
            for j in range(5):
                at = pl.ds(top + 5 * i + j, 8, stride=ROWS)
                stress[1, u, at, :] = w[i][j] * waves_ref[1, u, at, :]
    loads[6].wait()

    def backward(g, carry):
        inv_r = inv[pl.ds(8 * g, 8), :]
        at = [pl.ds(ROWS * c + 8 * g, 8) for c in range(8)]
        lhs = jnp.concatenate(
            [
                jnp.concatenate([stress[t, u, at[c], :] for t in range(2) for c in range(8)], axis=0)
                for u in range(2)
            ],
            axis=1,
        )
        out = jnp.dot(lhs.astype(jnp.bfloat16), back_ref[...], preferred_element_type=jnp.float32)
        terms = []
        for t in range(2):
            halves = []
            for half in range(2):
                v = []
                for c in range(8):
                    rows = out[64 * t + 8 * c : 64 * t + 8 * c + 8]
                    re = rows[:, LANES * half : LANES * (half + 1)]
                    im = rows[:, LANES * (2 + half) : LANES * (3 + half)]
                    if c:
                        k = 2 * c + half
                        cos, sin = twiddle_ref[k : k + 1, :], twiddle_ref[16 + k : 17 + k, :]
                        re, im = re * cos + im * sin, im * cos - re * sin
                    v.append((re, im))
                halves.append(gathered(v))
            terms.append([halves[a % 2][a // 2] for a in range(8)])
        for a in range(8):
            kept = (lane8 + 128 * a) < limit
            scale = orders[a]
            re = terms[0][a][0] + (scale * terms[1][a][1]) * inv_r
            im = terms[0][a][1] - (scale * terms[1][a][0]) * inv_r
            stiff_ref[pl.ds(128 * g + a, 8, stride=16), :] = jnp.where(kept, re, 0.0)
            stiff_ref[pl.ds(128 * g + 8 + a, 8, stride=16), :] = jnp.where(kept, im, 0.0)
        return carry

    for g in range(ROWS // 8):
        backward(g, 0)

    table_out[0, 0] = limit
    for side in range(2):
        table_out[0, 1 + side] = count_ref[0, side]
        table_out[0, 3 + side] = count_ref[0, 2 + side]
        for k in range(8):
            table_out[0, 8 + 8 * side + k] = blk_ref[side, k]
        for k in range(4):
            table_out[0, 24 + 4 * side + k] = band_ref[side, k]
    for n in range(NODES):
        growth_out[0, n] = scale_ref[0, n]
    sends = []
    for ids, side, slots, ref, hbm in (
        (blk_ref, 1 - odd, 8, even_ref, even_hbm), (blk_ref, odd, 8, odd_ref, odd_hbm),
        (band_ref, upper, 4, far_ref, far_hbm), (band_ref, 1 - upper, 4, chip_ref, chip_hbm),
    ):
        for k in range(slots):
            at = ids[side, k] * 16
            for f in range(2):
                ref[pl.ds((f * slots + k) * 16, 16), :] = stiff_ref[pl.ds(pl.multiple_of(at + 400 * f, 16), 16), :]
        sends.append(pltpu.make_async_copy(ref, hbm, sems.at[11 + len(sends)]))
        sends[-1].start()
    for load in loads[7:]:
        load.wait()

    @pl.when(first)
    def _():
        finish_locally(limit, scale_ref, waves_ref, stiff_ref, field, late, base_ref, slab, kout)
        store = pltpu.make_async_copy(kout.at[pl.ds(0, 400)], out_hbm, sems.at[10])
        store.start()
        store.wait()

    for send in sends:
        send.wait()


def local_kernel(
    numbers_ref, scale_ref, waves_ref, stiff_ref, field_ref, late_ref, base_in, out_in,
    base_ref, out_hbm, slab, kout, sem,
):
    first, _, _ = device_role()

    @pl.when(first)
    def _():
        base_ref[...] = base_in[...]

    @pl.when(jnp.logical_not(first))
    def _():
        limit = numbers_ref[0, 0]
        finish_locally(limit, scale_ref, waves_ref, stiff_ref, field_ref, late_ref, base_ref, slab, kout)
        store = pltpu.make_async_copy(kout.at[pl.ds(0, 400)], out_hbm, sem)
        store.start()
        store.wait()


def join_kernel(
    numbers_ref, scale_ref, base_ref, odd_ref, even_ref, chip_ref, far_ref, next_ref, last_ref,
    fwd_hbm, adj_hbm, total, sems,
):
    _, odd, upper = device_role()
    slot = lax.broadcasted_iota(jnp.int32, (16, LANES), 0)
    order = lax.broadcasted_iota(jnp.int32, (16, LANES), 1) + 128 * (slot % 8)
    kept = order < numbers_ref[0, 0]
    total[...] = base_ref[...]
    stores = []
    for f, out_hbm in enumerate((fwd_hbm, adj_hbm)):
        for start, ids, side, slots, got in (
            (1, 8, odd, 8, (odd_ref,)), (1, 8, 1 - odd, 8, (even_ref, next_ref)),
            (3, 24, 1 - upper, 4, (chip_ref,)), (3, 24, upper, 4, (far_ref, last_ref)),
        ):
            count = numbers_ref[0, start + side]
            for k in range(slots):
                node = numbers_ref[0, ids + slots * side + k]
                take = jnp.logical_and(kept, k < count)
                at = pl.ds(pl.multiple_of(16 * node + 400 * f, 16), 16)
                rows = pl.ds((f * slots + k) * 16, 16)
                step = scale_ref[0, node] * sum(ref[rows, :] for ref in got)
                total[at, :] = base_ref[at, :] - jnp.where(take, step, 0.0)
        stores.append(pltpu.make_async_copy(total.at[pl.ds(400 * f, 400)], out_hbm, sems.at[f]))
        stores[-1].start()
    for store in stores:
        store.wait()


def smem():
    return pl.BlockSpec(memory_space=pltpu.SMEM)


def vmem():
    return pl.BlockSpec(memory_space=pltpu.VMEM)


def anywhere():
    return pl.BlockSpec(memory_space=pl.ANY)


def near(*dims):
    return pltpu.VMEM(dims, jnp.float32)


def shape(*dims):
    return jax.ShapeDtypeStruct(dims, jnp.float32)


def swap(value, chosen):
    bands = lax.axis_size("band")
    pairs = [(b * bands + z, c * bands + y) for (b, z), (c, y) in chosen]
    pairs = sorted(pairs + [(target, source) for source, target in pairs])
    return lax.ppermute(value, ("blk", "band"), pairs)


def per_device(
    disp_fwd, prev_fwd, disp_adj, prev_adj, modulus, radius, step_scale, kernel_in, buckets, halo_count,
    blk_nodes, band_nodes,
):
    flat = lambda value: value.reshape(16 * NODES, LANES)
    inside = lambda value: pltpu.with_memory_space_constraint(value, pltpu.SMEM)
    close = lambda value: pltpu.with_memory_space_constraint(value, pltpu.VMEM)
    table, twiddle = transform_tables()
    bucket, blk, band = buckets.reshape(1, 1), blk_nodes.reshape(2, 8), band_nodes.reshape(2, 4)
    scale = step_scale.reshape(1, NODES)
    blks, bands = lax.axis_size("blk"), lax.axis_size("band")
    f32 = lambda *dims: pltpu.VMEM(dims, jnp.float32)
    stiff, waves, field, late, base, odd, even, chip, far, kernel_out, numbers, growth = pl.pallas_call(
        stiffness_kernel,
        out_shape=(
            near(16 * ROWS, LANES), near(2, 2, 8 * ROWS, LANES), near(16 * ROWS, LANES), near(1312, LANES),
            near(800, LANES), shape(256, LANES), shape(256, LANES), shape(128, LANES), shape(128, LANES), shape(400, LANES),
            pltpu.SMEM((1, 32), jnp.int32), pltpu.SMEM((1, NODES), jnp.float32),
        ),
        in_specs=[anywhere()] * 15,
        out_specs=(vmem(),) * 5 + (anywhere(),) * 5 + (smem(), smem()),
        scratch_shapes=[
            f32(512, LANES), f32(2, 8 * PITCH, LANES), f32(2, 2, 8 * ROWS, LANES), f32(ROWS, LANES), f32(32, LANES),
            pltpu.VMEM((512, 256), jnp.bfloat16), pltpu.VMEM((256, 512), jnp.bfloat16),
            f32(2, 8 * PITCH, LANES), f32(512, LANES), f32(256, LANES), f32(256, LANES), f32(128, LANES), f32(128, LANES),
            *SCALARS, pltpu.SemaphoreType.DMA((15,)), pltpu.SemaphoreType.DMA((6,)),
        ],
        cost_estimate=pl.CostEstimate(flops=500_000_000, bytes_accessed=3_000_000, transcendentals=0),
        name="stiffness",
    )(
        bucket, radius.reshape(1, NODES), scale, blk, band, halo_count.reshape(1, 4), jnp.asarray(twiddle, jnp.float32),
        jnp.asarray(table, jnp.bfloat16), jnp.asarray(table.T, jnp.bfloat16), flat(disp_fwd), flat(disp_adj),
        flat(modulus), flat(prev_fwd), flat(prev_adj), flat(kernel_in),
    )
    far_pairs = [((b, z), (b, z + 1)) for b in range(blks) for z in range(1, bands - 1, 2)]
    blk_pairs = [((b, z), (b + 1, z)) for b in range(blks - 1) for z in range(bands)]
    place = lambda pair: pair[0][0] % RUN
    even_pairs = [pair for pair in blk_pairs if pair[0][0] % 2 == 0]
    got_even = swap(even, [pair for pair in even_pairs if place(pair) < EARLY_EVEN])
    got_far = swap(far, [pair for pair in far_pairs if place(pair) < EARLY_FAR])
    got_odd = swap(odd, [pair for pair in blk_pairs if pair[0][0] % 2])
    got_chip = swap(chip, [((b, z), (b, z + 1)) for b in range(blks) for z in range(0, bands - 1, 2)])
    got_last = swap(far, [pair for pair in far_pairs if place(pair) >= EARLY_FAR])
    got_next = swap(even, [pair for pair in even_pairs if place(pair) >= EARLY_EVEN])
    base, kernel_out = pl.pallas_call(
        local_kernel,
        out_shape=(near(800, LANES), shape(400, LANES)),
        in_specs=[smem()] * 2 + [vmem()] * 5 + [anywhere()],
        out_specs=(vmem(), anywhere()),
        scratch_shapes=[f32(2, 8 * PITCH, LANES), f32(512, LANES), pltpu.SemaphoreType.DMA],
        input_output_aliases={6: 0, 7: 1},
        cost_estimate=pl.CostEstimate(flops=100_000_000, bytes_accessed=3_000_000, transcendentals=0),
        name="local",
    )(inside(numbers), inside(growth), close(waves), close(stiff), close(field), close(late), close(base), kernel_out)
    next_fwd, next_adj = pl.pallas_call(
        join_kernel,
        out_shape=(shape(400, LANES), shape(400, LANES)),
        in_specs=[smem()] * 2 + [vmem()] * 7,
        out_specs=(anywhere(), anywhere()),
        scratch_shapes=[f32(800, LANES), pltpu.SemaphoreType.DMA((2,))],
        cost_estimate=pl.CostEstimate(flops=1_000_000, bytes_accessed=1_500_000, transcendentals=0),
        name="join",
    )(
        inside(numbers), inside(growth), close(base), close(got_odd), close(got_even),
        close(got_chip), close(got_far), close(got_next), close(got_last),
    )
    return tuple(value.reshape(disp_fwd.shape) for value in (next_fwd, next_adj, kernel_out))


def solution(mesh):
    wide = P("blk", "band", None, None)
    line = P("blk", "band", None)
    in_specs = (wide,) * 5 + (line, line, wide, P("blk", "band"), line, wide, wide)

    return jax.shard_map(per_device, mesh=mesh, in_specs=in_specs, out_specs=(wide, wide, wide), check_vma=False)
```
